32 devices in a mesh: clip: 16 (over z, x, core), strip: 2 (over y).
Axes of the slice: x: 2, y: 2, z: 4, core: 2. Of those that a mesh axis runs over, the one named last changes fastest.
Arguments:
- video: bfloat16 [32, 2, 32, 32, 256], P('clip', None, 'strip')
- gain_first: float32 [256], replicated, may hold values from 0.1 to 1.9
- conv_weight: bfloat16 [3, 3, 3, 256, 256], replicated, may hold values from -0.078125 to 0.078125
- gain_second: float32 [256], replicated, may hold values from 0.1 to 1.9
- proj_weight: bfloat16 [256, 256], replicated, may hold values from -0.375 to 0.375
- codes: int32 [32, 2, 32, 32], P('clip', None, 'strip'), may hold values from 0 to 1023
- ema_sum: float32 [1024, 256], replicated, may hold values from -12 to 12
- ema_count: float32 [1024], replicated, may hold values from 0.5 to 8
Outputs:
- latent: float32 [32, 2, 32, 32, 256], P('clip', None, 'strip')
- codebook: float32 [1024, 256], replicated
- code_count: float32 [1024], replicated
- clip_error: float32 [32], P('clip')
The draws below stay inside these ranges and needn't reach their ends.
All inputs are finite; a program needn't handle non-finite values.
Results may differ from the reference program's by a relative error of at most 0.0029.
Values may be sent and summed in bfloat16 or wider, within the bound.
No kernel may reach another device: no remote copies, remote signals or barrier semaphores. Data moves between devices by JAX's collectives and lax.ppermute only.
A program may use at most 64 MiB of HBM per device.

```python
import math
import jax
import jax.numpy as jnp
import numpy as np
from jax import lax

FRAMES = 2
HGT = 32
WID = 32
CH = 256
EMB = 256
CODES = 1024
GROUPS = 32
CLIPS = 32


def draw_video(key, part):
    noise_key, scale_key = jax.random.split(jax.random.fold_in(key, 11), 2)
    row_scale = jnp.exp(jax.random.uniform(scale_key, (CLIPS, FRAMES, HGT, 1, 1), jnp.float32, 0.0, 2.3))
    values = jax.random.normal(noise_key, (CLIPS, FRAMES, HGT, WID, CH), jnp.float32) * row_scale
    return values.astype(jnp.bfloat16)


def with_ends(values, stream_key, low, high):
    spot = [jax.random.randint(jax.random.fold_in(stream_key, axis), (), 0, length) for axis, length in enumerate(values.shape)]
    longest = values.shape.index(max(values.shape))
    next_to = spot[:longest] + [(spot[longest] + 1) % values.shape[longest]] + spot[longest + 1:]
    return values.at[tuple(spot)].set(low).at[tuple(next_to)].set(high)


def rank_bounds(number_of, lean):
    weights = [(1 << 20) // math.isqrt(grade ** lean) + 1 for grade in range(1, number_of + 1)]
    deviation = 1 + sum(weights) // (1 << 30)
    return np.cumsum(np.array([max(1, weight // deviation) for weight in weights]))


def skewed_ids(rng, extent, count, skew):
    listing = rank_bounds(count, skew)
    pick = jax.random.randint(jax.random.fold_in(rng, 1), extent, 0, int(listing[count - 1]))
    rank = jnp.searchsorted(jnp.asarray(listing, jnp.int32), pick, side="right")
    return jax.random.permutation(jax.random.fold_in(rng, 2), count)[rank].astype(jnp.int32)


def scatter_about(stream_key, extent, deviation, limit, held_as=jnp.bfloat16):
    drawn = jax.random.normal(stream_key, extent, jnp.float32) * deviation
    return jnp.minimum(jnp.maximum(drawn, -limit), limit).astype(held_as)


def setup_inputs(seed: int = 0) -> dict:
    seeds = jax.random.split(jax.random.key(seed), 9)
    return {
        "video": draw_video(jax.random.fold_in(seeds[8], 71), 0),
        "gain_first": jnp.clip(1.0 + 0.18 * jax.random.normal(seeds[1], (CH,), jnp.float32), 0.1, 1.9),
        "conv_weight": scatter_about(seeds[2], (3, 3, 3, CH, CH), (27 * CH) ** -0.5, 0.078125),
        "gain_second": jnp.clip(1.0 + 0.18 * jax.random.normal(seeds[3], (CH,), jnp.float32), 0.1, 1.9),
        "proj_weight": scatter_about(seeds[4], (CH, EMB), CH ** -0.5, 0.375),
        "codes": with_ends(skewed_ids(seeds[5], (CLIPS, FRAMES, HGT, WID), CODES, 3), jax.random.fold_in(seeds[5], 3), 0, CODES - 1).astype(jnp.int32),
        "ema_sum": scatter_about(seeds[6], (CODES, EMB), 2.0, 12.0, jnp.float32),
        "ema_count": jnp.clip(jnp.exp(jax.random.uniform(seeds[7], (CODES,), jnp.float32, math.log(0.5), math.log(8.0))), 0.5, 8.0),
    }


norm_eps = 1e-06
smooth_eps = 1e-05
ema_decay = 0.9

def group_norm(values, gain_vec):
    shaped = values.reshape(values.shape[:4] + (GROUPS, values.shape[4] // GROUPS))
    centre = lax.optimization_barrier(jnp.mean(shaped, axis=(1, 2, 3, 5), keepdims=True))
    spread = lax.optimization_barrier(jnp.mean((shaped - centre) ** 2, axis=(1, 2, 3, 5), keepdims=True))
    normed = (shaped - centre) / jnp.sqrt(spread + norm_eps)
    return normed.reshape(values.shape) * gain_vec

def smoothed_book(sums, counts):
    grand = jnp.sum(counts)
    smooth = (counts + smooth_eps) / (grand + CODES * smooth_eps) * grand
    return sums / smooth[:, None]

def reference(video, gain_first, conv_weight, gain_second, proj_weight, codes, ema_sum, ema_count):
    values = video.astype(jnp.float32)
    act_first = jax.nn.silu(group_norm(values, gain_first)).astype(jnp.bfloat16)
    convolved = lax.conv_general_dilated(act_first, conv_weight, (1, 1, 1), [(2, 0), (1, 1), (1, 1)], dimension_numbers=('NDHWC', 'DHWIO', 'NDHWC'), preferred_element_type=jnp.float32)
    hidden = values + convolved
    act_second = jax.nn.silu(group_norm(hidden, gain_second)).astype(jnp.bfloat16)
    flat_latent = jnp.dot(act_second.reshape(-1, CH), proj_weight, preferred_element_type=jnp.float32)
    flat_codes = codes.reshape(-1)
    old_book = smoothed_book(ema_sum, ema_count)
    quantized = jnp.take(old_book, flat_codes, axis=0)
    squared = lax.optimization_barrier(jnp.sum((flat_latent - quantized) ** 2, axis=1)).reshape(CLIPS, -1)
    clip_error = lax.optimization_barrier(jnp.sum(squared, axis=1)) / (squared.shape[1] * EMB)
    code_sums = jax.ops.segment_sum(flat_latent, flat_codes, CODES)
    token_counts = jax.ops.segment_sum(jnp.ones(flat_codes.shape, jnp.float32), flat_codes, CODES)
    code_count = ema_decay * ema_count + (1.0 - ema_decay) * token_counts
    new_sum = ema_decay * ema_sum + (1.0 - ema_decay) * code_sums
    codebook = smoothed_book(new_sum, code_count)
    latent = flat_latent.reshape(CLIPS, FRAMES, HGT, WID, EMB)
    return (latent, codebook, code_count, clip_error)
```

```python
import functools

import jax
import jax.numpy as jnp
from jax import lax
from jax.experimental import pallas as pl
from jax.experimental.pallas import tpu as pltpu
from jax.sharding import PartitionSpec as P

GROUPS = 32

norm_eps = 1e-06
smooth_eps = 1e-05
ema_decay = 0.9

f32 = jnp.float32
bf16 = jnp.bfloat16
LANES = 128
SHARDS = 8
TAIL = 8
BOTH = ("clip", "strip")
VMEM = pltpu.VMEM
VSPEC = pl.BlockSpec(memory_space=pltpu.VMEM)


def call(kernel, outs, args, scratch=(), flops=0, limit=None, name=None):
    return pl.pallas_call(
        kernel,
        out_shape=tuple(jax.ShapeDtypeStruct(s, d) for s, d in outs),
        in_specs=[VSPEC] * len(args),
        out_specs=tuple(VSPEC for _ in outs),
        scratch_shapes=list(scratch),
        compiler_params=pltpu.CompilerParams(vmem_limit_bytes=limit),
        cost_estimate=pl.CostEstimate(flops=flops, bytes_accessed=0, transcendentals=0),
        name=name,
    )(*args)


def pieces(value):
    head = value.astype(bf16)
    rest = value - head.astype(f32)
    middle = rest.astype(bf16)
    last = (rest - middle.astype(f32)).astype(bf16)
    return head, middle, last


def group_matrix(channels):
    shift = (channels // GROUPS).bit_length() - 1
    rows = lax.broadcasted_iota(jnp.int32, (channels, channels), 0) >> shift
    cols = lax.broadcasted_iota(jnp.int32, (channels, channels), 1) >> shift
    return jnp.where(rows == cols, 1.0, 0.0).astype(f32)


def group_total(rows, matrix):
    return jnp.dot(rows, matrix, precision=lax.Precision.HIGHEST, preferred_element_type=f32)


def stacked(rows, channels):
    row = lax.broadcasted_iota(jnp.int32, (8, channels), 0)
    out = jnp.zeros((8, channels), f32)
    for i, value in enumerate(rows):
        out = jnp.where(row == i, value, out)
    return out


def local_stats(read, clips, blocks, rows, channels):
    matrix = group_matrix(channels)
    members = blocks * rows * (channels // GROUPS)
    sums = []
    for c in range(clips):
        total = lax.fori_loop(
            0, blocks, lambda i, acc: acc + read(c, i), jnp.zeros((rows, channels), f32), unroll=4
        )
        sums.append(jnp.sum(total, axis=0, keepdims=True))
    means = group_total(stacked(sums, channels), matrix) / members
    squares = []
    for c in range(clips):
        mean = means[c : c + 1]

        def step(i, acc):
            away = read(c, i) - mean
            return acc + away * away

        total = lax.fori_loop(0, blocks, step, jnp.zeros((rows, channels), f32), unroll=4)
        squares.append(jnp.sum(total, axis=0, keepdims=True))
    squares = group_total(stacked(squares, channels), matrix)
    return means, squares, members


def merged(mean_a, square_a, mean_b, square_b, members):
    mean = 0.5 * (mean_a + mean_b)
    apart = mean_a - mean_b
    spread = (square_a + square_b + apart * apart * (0.5 * members)) / (2 * members)
    return mean, lax.rsqrt(spread + norm_eps)


def silu(v):
    half = 0.5 * v
    return half + half * jnp.tanh(half)


def stats_kernel(video_ref, pay_ref, loc_ref):
    clips, frames, rows, cols, channels = video_ref.shape
    strip = lax.axis_index("strip")
    edge = (1 - strip) * (rows - 1)
    for c in range(clips):
        for t in range(frames):
            at = (c * frames + t) * cols
            pay_ref[at : at + cols] = video_ref[c, t, edge]

    def read(c, i):
        return video_ref[c, i // rows, i % rows].astype(f32)

    means, squares, _ = local_stats(read, clips, frames * rows, cols, channels)
    loc_ref[0:8] = means
    loc_ref[8:16] = squares
    base = clips * frames * cols
    row = lax.broadcasted_iota(jnp.int32, (16, channels), 0)
    out = jnp.zeros((16, channels), f32)
    for j, value in enumerate((means, squares)):
        for k, piece in enumerate(pieces(value)):
            piece = piece.astype(f32)
            for c in range(clips):
                out = jnp.where(row == (j * clips + c) * 3 + k, piece[c : c + 1], out)
    pay_ref[base : base + 16] = out.astype(bf16)


def conv_kernel(video_ref, pay_ref, loc_ref, gain_ref, w_ref, hid_ref, st_ref, buf_ref):
    clips, frames, rows, cols, channels = video_ref.shape
    strip = lax.axis_index("strip")
    members = frames * rows * cols * (channels // GROUPS)
    base = clips * frames * cols
    far = pay_ref[base : base + 16].astype(f32)
    gain = gain_ref[...]
    col = lax.broadcasted_iota(jnp.int32, (cols, channels), 0)

    def put(c, t, r, act):
        left = jnp.where(col == 0, 0.0, pltpu.roll(act, 1, 0))
        right = jnp.where(col == cols - 1, 0.0, pltpu.roll(act, cols - 1, 0))
        buf_ref[c, t, r, :, 0:channels] = left.astype(bf16)
        buf_ref[c, t, r, :, channels : 2 * channels] = act.astype(bf16)
        buf_ref[c, t, r, :, 2 * channels : 3 * channels] = right.astype(bf16)

    for c in range(clips):
        at = [(j * clips + c) * 3 for j in (0, 1)]
        far_mean, far_square = [far[i : i + 1] + far[i + 1 : i + 2] + far[i + 2 : i + 3] for i in at]
        mean, inverse = merged(
            loc_ref[c : c + 1], loc_ref[8 + c : 9 + c], far_mean, far_square, members
        )
        scale = inverse * gain
        for t in range(frames):
            def row_step(r, carry):
                x = video_ref[c, t, r].astype(f32)
                put(c, t, r + 1, silu((x - mean) * scale))
                return carry

            lax.fori_loop(0, rows, row_step, 0, unroll=4)
            where_at = (c * frames + t) * cols
            halo = silu((pay_ref[where_at : where_at + cols].astype(f32) - mean) * scale)
            put(c, t, 0, jnp.where(strip > 0, halo, 0.0))
            put(c, t, rows + 1, jnp.where(strip > 0, 0.0, halo))

        def patches(t):
            return jnp.concatenate(
                [
                    buf_ref[c, t, b : b + rows].reshape(rows * cols, 3 * channels)
                    for b in range(3)
                ],
                axis=1,
            )

        for t in range(frames):
            total = video_ref[c, t].reshape(rows * cols, channels).astype(f32)
            for a in range(3):
                if t + a - 2 >= 0:
                    total = total + jnp.dot(
                        patches(t + a - 2), w_ref[a], preferred_element_type=f32
                    )
            hid_ref[c, t * rows * cols : (t + 1) * rows * cols] = total

    def read(c, i):
        return hid_ref[c, pl.ds(pl.multiple_of(i * cols, cols), cols)]

    means, squares, _ = local_stats(read, clips, frames * rows, cols, channels)
    st_ref[0:8] = means
    st_ref[8:16] = squares


def shard_bits():
    clip = lax.axis_index("clip")
    return ((clip & 1) << 2) | (((clip >> 1) & 1) << 1) | lax.axis_index("strip")


def tail_rows(count, extra=None):
    row = lax.broadcasted_iota(jnp.int32, (TAIL, 2 * LANES), 0)
    zero = jnp.zeros((1, LANES), f32)
    out = jnp.zeros((TAIL, 2 * LANES), f32)
    for i, value in enumerate((count,) if extra is None else (count, extra)):
        head, middle, last = [p.astype(f32) for p in pieces(value)]
        out = jnp.where(row == 2 * i, jnp.concatenate([head, middle], axis=1), out)
        out = jnp.where(row == 2 * i + 1, jnp.concatenate([last, zero], axis=1), out)
    return out.astype(bf16)


def untail(block, which=0):
    block = block.astype(f32)
    i = 2 * which
    return (
        block[i : i + 1, :LANES] + block[i : i + 1, LANES:] + block[i + 1 : i + 2, :LANES]
    )


def segment_kernel(
    hid_ref, near_ref, far_ref, gain_ref, codes_ref, act_ref, send_ref, keep_ref, cnt_ref, acc_ref
):
    clips, tokens, channels = hid_ref.shape
    members = tokens * (channels // GROUPS)
    gain = gain_ref[...]
    block = 64
    for c in range(clips):
        mean, inverse = merged(
            near_ref[c : c + 1],
            near_ref[8 + c : 9 + c],
            far_ref[c : c + 1],
            far_ref[8 + c : 9 + c],
            members,
        )
        scale = inverse * gain

        def step(i, carry):
            x = hid_ref[c, pl.ds(pl.multiple_of(i * block, block), block)]
            act = silu((x - mean) * scale).astype(bf16)
            act_ref[pl.ds(pl.multiple_of(c * tokens + i * block, block), block)] = act
            return carry

        lax.fori_loop(0, tokens // block, step, 0, unroll=2)

    me = shard_bits()
    codes_count = acc_ref.shape[0]
    share = codes_count // SHARDS
    codes = codes_ref[...] ^ (me * share)
    row_code = lax.broadcasted_iota(jnp.int32, (codes_count, LANES), 0)
    low_code = lax.broadcasted_iota(jnp.int32, (share, LANES), 0)
    high_code = lax.broadcasted_iota(jnp.int32, (SHARDS, LANES), 0)
    count = jnp.zeros((SHARDS, LANES), f32)
    width = 2
    shift = share.bit_length() - 1
    for k in range(codes.shape[0] // width):
        hot = []
        for j in range(width):
            line = codes[k * width + j : k * width + j + 1]
            hot.append(jnp.where(row_code == line, 1.0, 0.0).astype(bf16))
            low = jnp.where(low_code == (line & (share - 1)), 1.0, 0.0).astype(bf16)
            high = jnp.where(high_code == (line >> shift), 1.0, 0.0).astype(bf16)
            count = count + lax.dot_general(
                high, low, (((1,), (1,)), ((), ())), preferred_element_type=f32
            )
        part = jnp.dot(
            jnp.concatenate(hot, axis=1),
            act_ref[k * width * LANES : (k + 1) * width * LANES],
            preferred_element_type=f32,
        )
        if k == 0:
            acc_ref[...] = part
        else:
            acc_ref[...] += part
    cnt_ref[...] = count
    half = SHARDS // 2
    keep_ref[...] = acc_ref[: half * share].reshape(half, share, channels)
    for p in range(half):
        send_ref[p, :share] = acc_ref[(half + p) * share : (half + p + 1) * share].astype(bf16)
        send_ref[p, share:] = tail_rows(count[half + p : half + p + 1])


def quarter_kernel(keep_ref, cnt_ref, got_ref, mine_ref, mcnt_ref, s1_ref, s2_ref, s3_ref):
    share = keep_ref.shape[1]
    for p, out in enumerate((None, s1_ref, s2_ref, s3_ref)):
        value = keep_ref[p] + got_ref[p, :share].astype(f32)
        count = cnt_ref[p : p + 1] + untail(got_ref[p, share:])
        if out is None:
            mine_ref[...] = value
            mcnt_ref[...] = jnp.broadcast_to(count, (8, LANES))
        else:
            out[:share] = value.astype(bf16)
            out[share:] = tail_rows(count)


def gathered_kernel(mine_ref, mcnt_ref, a_ref, b_ref, c_ref, out_ref):
    share = mine_ref.shape[0]
    value = mine_ref[...]
    count = mcnt_ref[0:1]
    for ref in (a_ref, b_ref, c_ref):
        value = value + ref[:share].astype(f32)
        count = count + untail(ref[share:])
    out_ref[:share] = value.astype(bf16)
    out_ref[share:] = tail_rows(count)


def pair_kernel(own_ref, got_ref, out_ref):
    share = own_ref.shape[0] - TAIL
    value = own_ref[:share].astype(f32) + got_ref[:share].astype(f32)
    out_ref[:share] = value.astype(bf16)
    out_ref[share:] = tail_rows(untail(own_ref[share:]) + untail(got_ref[share:]))


def project_kernel(own_ref, got_ref, w_ref, err_ref, out_ref):
    share = own_ref.shape[0] - TAIL
    value = own_ref[:share].astype(f32) + got_ref[:share].astype(f32)
    head = value.astype(bf16)
    rest = (value - head.astype(f32)).astype(bf16)
    sums = jnp.dot(head, w_ref[...], preferred_element_type=f32) + jnp.dot(
        rest, w_ref[...], preferred_element_type=f32
    )
    out_ref[:share] = sums.astype(bf16)
    out_ref[share:] = tail_rows(
        untail(own_ref[share:]) + untail(got_ref[share:]), err_ref[0:1]
    )


def as_column(row):
    return jnp.transpose(jnp.broadcast_to(row, (LANES, LANES)))


def latent_kernel(act_ref, w_ref, codes_ref, sum_ref, cnt_ref, lat_ref, err_ref, head_ref, rest_ref):
    tokens, channels = lat_ref.shape
    codes_count = sum_ref.shape[0]
    clips = 2
    counts = cnt_ref[...]
    grand = jnp.sum(counts)
    smooth = (counts + smooth_eps) / (grand + codes_count * smooth_eps) * grand
    for i in range(codes_count // LANES):
        divisor = as_column(smooth[i : i + 1])
        divisor = jnp.concatenate([divisor] * (channels // LANES), axis=1)
        book = sum_ref[i * LANES : (i + 1) * LANES] / divisor
        head = book.astype(bf16)
        head_ref[i * LANES : (i + 1) * LANES] = head
        rest_ref[i * LANES : (i + 1) * LANES] = (book - head.astype(f32)).astype(bf16)
    lane_code = lax.broadcasted_iota(jnp.int32, (LANES, codes_count), 1)
    lane = lax.broadcasted_iota(jnp.int32, (1, LANES), 1)
    lines = tokens // LANES
    per_clip = lines // clips
    errors = jnp.zeros((1, LANES), f32)
    for c in range(clips):
        def step(i, acc):
            line = c * per_clip + i
            at = pl.ds(pl.multiple_of(line * LANES, LANES), LANES)
            latent = jnp.dot(act_ref[at], w_ref[...], preferred_element_type=f32)
            lat_ref[at] = latent
            column = as_column(codes_ref[pl.ds(line, 1)])
            column = jnp.concatenate([column] * (codes_count // LANES), axis=1)
            hot = jnp.where(column == lane_code, 1.0, 0.0).astype(bf16)
            chosen = jnp.dot(hot, head_ref[...], preferred_element_type=f32) + jnp.dot(
                hot, rest_ref[...], preferred_element_type=f32
            )
            away = latent - chosen
            away = away * away
            return acc + jnp.sum(away.reshape(LANES // 8, 8, channels), axis=0)

        total = lax.fori_loop(0, per_clip, step, jnp.zeros((8, channels), f32), unroll=2)
        errors = jnp.where(lane == c, jnp.sum(total), errors)
    err_ref[...] = jnp.broadcast_to(errors, (8, LANES))


def final_kernel(scale, tokens, p0, p1, p2, p3, q_ref, sum_ref, cnt_ref, err_ref, book_ref, count_ref, error_ref):
    share = LANES
    me = shard_bits()
    grand = ema_decay * jnp.sum(cnt_ref[...]) + (1.0 - ema_decay) * tokens
    for p in range(SHARDS):
        src = (p0, p1, p2, p3)[p] if p < 4 else q_ref.at[p - 4]
        shard = p ^ me
        count = ema_decay * cnt_ref[pl.ds(shard, 1)] + (1.0 - ema_decay) * untail(src[share:])
        count_ref[pl.ds(shard, 1)] = count
        smooth = (count + smooth_eps) / (grand + SHARDS * share * smooth_eps) * grand
        divisor = as_column(smooth)
        channels = book_ref.shape[1]
        divisor = jnp.concatenate([divisor] * (channels // LANES), axis=1)
        at = pl.ds(pl.multiple_of(shard * share, share), share)
        fresh = ema_decay * sum_ref[at] + (1.0 - ema_decay) * src[:share].astype(f32)
        book_ref[at] = fresh / divisor
    error_ref[...] = jnp.broadcast_to((err_ref[0:1] + untail(p1[share:], 1)) * scale, (8, LANES))


def body(video, gain_first, conv_weight, gain_second, proj_weight, codes, ema_sum, ema_count):
    clips, frames, rows, cols, channels = video.shape
    codes_count = ema_sum.shape[0]
    clip_size, strips = lax.axis_size("clip"), lax.axis_size("strip")
    n = clip_size * strips
    share = codes_count // SHARDS
    assert strips == 2 and clip_size >= 4 and clip_size & (clip_size - 1) == 0
    assert share == LANES and channels == 2 * LANES and clips == 2

    def swap(x, mask):
        return lax.ppermute(x, BOTH, [(i, i ^ mask) for i in range(n)])

    tokens = frames * rows * cols
    halo = clips * frames * cols
    pay, near = call(
        stats_kernel,
        [((halo + 16, channels), bf16), ((16, channels), f32)],
        [video],
        flops=10_000_000,
        limit=8 << 20,
        name="stats",
    )
    far_pay = swap(pay, 1)
    code_lines = codes.reshape(-1, LANES)
    weights = conv_weight.reshape(3, 9 * channels, channels)
    hidden, near_two = call(
        conv_kernel,
        [((clips, tokens, channels), f32), ((16, channels), f32)],
        [video, far_pay, near, gain_first.reshape(1, channels), weights],
        scratch=[VMEM((clips, frames, rows + 2, cols, 3 * channels), bf16)],
        flops=4_000_000_000,
        limit=24 << 20,
        name="conv",
    )
    far_two = swap(near_two, 1)
    act, send, keep, cnt = call(
        segment_kernel,
        [
            ((clips * tokens, channels), bf16),
            ((SHARDS // 2, share + TAIL, channels), bf16),
            ((SHARDS // 2, share, channels), f32),
            ((SHARDS, LANES), f32),
        ],
        [hidden, near_two, far_two, gain_second.reshape(1, channels), code_lines],
        scratch=[VMEM((codes_count, channels), f32)],
        flops=1_500_000_000,
        limit=24 << 20,
        name="segment",
    )
    core, x_bit = 2, 4
    got = swap(send, core)
    counts = ema_count.reshape(SHARDS, LANES)
    latent, err = call(
        latent_kernel,
        [((clips * tokens, channels), f32), ((8, LANES), f32)],
        [act, proj_weight, code_lines, ema_sum, counts],
        scratch=[VMEM((codes_count, channels), bf16)] * 2,
        flops=2_500_000_000,
        limit=24 << 20,
        name="latent",
    )
    flat = ((share + TAIL, channels), bf16)
    mine, mine_cnt, s1, s2, s3 = call(
        quarter_kernel,
        [((share, channels), f32), ((8, LANES), f32), flat, flat, flat],
        [keep, cnt, got],
        flops=1_000_000,
        limit=8 << 20,
        name="quarter",
    )
    near_masks = (1, x_bit, 1 | x_bit)
    parts = [swap(s, m) for s, m in zip((s1, s2, s3), near_masks)]
    (own,) = call(
        gathered_kernel, [flat], [mine, mine_cnt, *parts], flops=1_000_000, limit=8 << 20, name="gathered"
    )
    bit = 8
    while bit < n // 2:
        (own,) = call(
            pair_kernel, [flat], [own, swap(own, bit)], flops=1_000_000, limit=8 << 20, name="pair"
        )
        bit *= 2
    last = swap(own, bit) if bit < n else jnp.zeros_like(own)
    (done,) = call(
        project_kernel, [flat], [own, last, proj_weight, err], flops=1_000_000, limit=8 << 20, name="project"
    )
    peers = [swap(done, m) for m in near_masks]
    across = swap(jnp.stack([done, *peers]), core)
    scale = 1.0 / (tokens * strips * channels)
    book, count, error = call(
        functools.partial(final_kernel, scale, float(clips * tokens * n)),
        [((codes_count, channels), f32), ((SHARDS, LANES), f32), ((8, LANES), f32)],
        [done, *peers, across, ema_sum, counts, err],
        flops=1_000_000,
        limit=8 << 20,
        name="final",
    )
    return (
        latent.reshape(clips, frames, rows, cols, channels),
        book,
        count.reshape(codes_count),
        error[0, :clips],
    )


def solution(mesh):
    in_specs = (
        P("clip", None, "strip", None, None),
        P(),
        P(),
        P(),
        P(),
        P("clip", None, "strip", None),
        P(),
        P(),
    )
    out_specs = (P("clip", None, "strip", None, None), P(), P(), P("clip"))
    return jax.shard_map(body, mesh=mesh, in_specs=in_specs, out_specs=out_specs, check_vma=False)
```

```python
import functools

import jax
import jax.numpy as jnp
from jax import lax
from jax.experimental import pallas as pl
from jax.experimental.pallas import tpu as pltpu
from jax.sharding import PartitionSpec as P

GROUPS = 32

norm_eps = 1e-06
smooth_eps = 1e-05
ema_decay = 0.9

f32 = jnp.float32
bf16 = jnp.bfloat16
LANES = 128
SHARDS = 8
TAIL = 8
BOTH = ("clip", "strip")
VMEM = pltpu.VMEM
VSPEC = pl.BlockSpec(memory_space=pltpu.VMEM)


def call(kernel, outs, args, scratch=(), flops=0, limit=None, name=None, far=(), far_outs=(), alias=None):
    far_spec = pl.BlockSpec(memory_space=pltpu.HBM)
    return pl.pallas_call(
        kernel,
        out_shape=tuple(jax.ShapeDtypeStruct(s, d) for s, d in outs),
        in_specs=[far_spec if i in far else VSPEC for i in range(len(args))],
        out_specs=tuple(far_spec if i in far_outs else VSPEC for i in range(len(outs))),
        scratch_shapes=list(scratch),
        input_output_aliases=alias or {},
        compiler_params=pltpu.CompilerParams(vmem_limit_bytes=limit),
        cost_estimate=pl.CostEstimate(flops=flops, bytes_accessed=0, transcendentals=0),
        name=name,
    )(*args)


def pieces(value):
    head = value.astype(bf16)
    rest = value - head.astype(f32)
    middle = rest.astype(bf16)
    last = (rest - middle.astype(f32)).astype(bf16)
    return head, middle, last


def group_matrix(channels):
    shift = (channels // GROUPS).bit_length() - 1
    rows = lax.broadcasted_iota(jnp.int32, (channels, channels), 0) >> shift
    cols = lax.broadcasted_iota(jnp.int32, (channels, channels), 1) >> shift
    return jnp.where(rows == cols, 1.0, 0.0).astype(bf16)


def group_total(rows, matrix):
    split = [p.astype(f32) for p in pieces(rows)]
    split = jnp.concatenate(split + [jnp.zeros_like(rows)], axis=0).astype(bf16)
    total = jnp.dot(split, matrix, preferred_element_type=f32)
    return total[0:8] + total[8:16] + total[16:24]


def stacked(rows, channels):
    row = lax.broadcasted_iota(jnp.int32, (8, channels), 0)
    out = jnp.zeros((8, channels), f32)
    for i, value in enumerate(rows):
        out = jnp.where(row == i, value, out)
    return out


def local_stats(read, clips, blocks, rows, channels):
    matrix = group_matrix(channels)
    members = blocks * rows * (channels // GROUPS)
    sums = []
    for c in range(clips):
        total = lax.fori_loop(
            0, blocks, lambda i, acc: acc + read(c, i), jnp.zeros((rows, channels), f32), unroll=8
        )
        sums.append(jnp.sum(total, axis=0, keepdims=True))
    means = group_total(stacked(sums, channels), matrix) / members
    squares = []
    for c in range(clips):
        mean = means[c : c + 1]

        def step(i, acc):
            away = read(c, i) - mean
            return acc + away * away

        total = lax.fori_loop(0, blocks, step, jnp.zeros((rows, channels), f32), unroll=8)
        squares.append(jnp.sum(total, axis=0, keepdims=True))
    squares = group_total(stacked(squares, channels), matrix)
    return means, squares, members


def merged(mean_a, square_a, mean_b, square_b, members):
    mean = 0.5 * (mean_a + mean_b)
    apart = mean_a - mean_b
    spread = (square_a + square_b + apart * apart * (0.5 * members)) / (2 * members)
    return mean, lax.rsqrt(spread + norm_eps)


def silu(v):
    half = 0.5 * v
    return half + half * jnp.tanh(half)


def stats_kernel(video_hbm, w_hbm, pay_ref, loc_ref, video_ref, w_ref, sems):
    clips, frames, rows, cols, channels = video_ref.shape
    strip = lax.axis_index("strip")
    loads = [
        pltpu.make_async_copy(video_hbm.at[c], video_ref.at[c], sems.at[c]) for c in range(clips)
    ]
    first_tap = w_hbm.shape[0] - w_ref.shape[0]
    taps = pltpu.make_async_copy(w_hbm.at[pl.ds(first_tap, w_ref.shape[0])], w_ref, sems.at[clips])
    for load in loads:
        load.start()
    taps.start()
    for load in loads:
        load.wait()
    edge = (1 - strip) * (rows - 1)
    for c in range(clips):
        for t in range(frames):
            at = (c * frames + t) * cols
            pay_ref[at : at + cols] = video_ref[c, t, edge]

    def read(c, i):
        return video_ref[c, i // rows, i % rows].astype(f32)

    means, squares, _ = local_stats(read, clips, frames * rows, cols, channels)
    loc_ref[0:8] = means
    loc_ref[8:16] = squares
    base = clips * frames * cols
    row = lax.broadcasted_iota(jnp.int32, (16, channels), 0)
    out = jnp.zeros((16, channels), f32)
    for j, value in enumerate((means, squares)):
        for k, piece in enumerate(pieces(value)):
            piece = piece.astype(f32)
            for c in range(clips):
                out = jnp.where(row == (j * clips + c) * 3 + k, piece[c : c + 1], out)
    pay_ref[base : base + 16] = out.astype(bf16)
    taps.wait()


def conv_kernel(video_ref, pay_ref, loc_ref, gain_ref, w_ref, hid_ref, st_ref, buf_ref):
    clips, frames, rows, cols, channels = video_ref.shape
    strip = lax.axis_index("strip")
    members = frames * rows * cols * (channels // GROUPS)
    base = clips * frames * cols
    first_tap = 3 - w_ref.shape[0]
    far = pay_ref[base : base + 16].astype(f32)
    gain = gain_ref[...]
    col = lax.broadcasted_iota(jnp.int32, (cols, channels), 0)

    def put(c, t, r, act):
        left = jnp.where(col == 0, 0.0, pltpu.roll(act, 1, 0))
        right = jnp.where(col == cols - 1, 0.0, pltpu.roll(act, cols - 1, 0))
        buf_ref[c, t, r, :, 0:channels] = left.astype(bf16)
        buf_ref[c, t, r, :, channels : 2 * channels] = act.astype(bf16)
        buf_ref[c, t, r, :, 2 * channels : 3 * channels] = right.astype(bf16)

    for c in range(clips):
        at = [(j * clips + c) * 3 for j in (0, 1)]
        far_mean, far_square = [far[i : i + 1] + far[i + 1 : i + 2] + far[i + 2 : i + 3] for i in at]
        mean, inverse = merged(
            loc_ref[c : c + 1], loc_ref[8 + c : 9 + c], far_mean, far_square, members
        )
        scale = inverse * gain
        for t in range(frames):
            def row_step(r, carry):
                x = video_ref[c, t, r].astype(f32)
                put(c, t, r + 1, silu((x - mean) * scale))
                return carry

            lax.fori_loop(0, rows, row_step, 0, unroll=True)
            where_at = (c * frames + t) * cols
            halo = silu((pay_ref[where_at : where_at + cols].astype(f32) - mean) * scale)
            put(c, t, 0, jnp.where(strip > 0, halo, 0.0))
            put(c, t, rows + 1, jnp.where(strip > 0, 0.0, halo))

        def patches(t):
            return jnp.concatenate(
                [
                    buf_ref[c, t, b : b + rows].reshape(rows * cols, 3 * channels)
                    for b in range(3)
                ],
                axis=1,
            )

        for t in range(frames):
            total = video_ref[c, t].reshape(rows * cols, channels).astype(f32)
            for a in range(3):
                if t + a - 2 >= 0:
                    total = total + jnp.dot(
                        patches(t + a - 2), w_ref[a - first_tap], preferred_element_type=f32
                    )
            hid_ref[c, t * rows * cols : (t + 1) * rows * cols] = total

    def read(c, i):
        return hid_ref[c, pl.ds(pl.multiple_of(i * cols, cols), cols)]

    means, squares, _ = local_stats(read, clips, frames * rows, cols, channels)
    st_ref[0:8] = means
    st_ref[8:16] = squares


def shard_bits():
    clip = lax.axis_index("clip")
    return ((clip & 1) << 2) | (((clip >> 1) & 1) << 1) | lax.axis_index("strip")


def tail_rows(count, extra=None):
    row = lax.broadcasted_iota(jnp.int32, (TAIL, 2 * LANES), 0)
    zero = jnp.zeros((1, LANES), f32)
    out = jnp.zeros((TAIL, 2 * LANES), f32)
    for i, value in enumerate((count,) if extra is None else (count, extra)):
        head, middle, last = [p.astype(f32) for p in pieces(value)]
        out = jnp.where(row == 2 * i, jnp.concatenate([head, middle], axis=1), out)
        out = jnp.where(row == 2 * i + 1, jnp.concatenate([last, zero], axis=1), out)
    return out.astype(bf16)


def untail(block, which=0):
    block = block.astype(f32)
    i = 2 * which
    return (
        block[i : i + 1, :LANES] + block[i : i + 1, LANES:] + block[i + 1 : i + 2, :LANES]
    )


def segment_kernel(
    hid_ref, near_ref, far_ref, gain_ref, codes_ref, act_ref, send_ref, keep_ref, cnt_ref, acc_ref
):
    clips, tokens, channels = hid_ref.shape
    members = tokens * (channels // GROUPS)
    gain = gain_ref[...]
    block = 64
    for c in range(clips):
        mean, inverse = merged(
            near_ref[c : c + 1],
            near_ref[8 + c : 9 + c],
            far_ref[c : c + 1],
            far_ref[8 + c : 9 + c],
            members,
        )
        scale = inverse * gain

        def step(i, carry):
            x = hid_ref[c, pl.ds(pl.multiple_of(i * block, block), block)]
            act = silu((x - mean) * scale).astype(bf16)
            act_ref[pl.ds(pl.multiple_of(c * tokens + i * block, block), block)] = act
            return carry

        lax.fori_loop(0, tokens // block, step, 0, unroll=True)

    me = shard_bits()
    codes_count = acc_ref.shape[0]
    share = codes_count // SHARDS
    codes = codes_ref[...] ^ (me * share)
    row_code = lax.broadcasted_iota(jnp.int32, (codes_count, LANES), 0)
    low_code = lax.broadcasted_iota(jnp.int32, (share, LANES), 0)
    high_code = lax.broadcasted_iota(jnp.int32, (SHARDS, LANES), 0)
    count = jnp.zeros((SHARDS, LANES), f32)
    width = 2
    shift = share.bit_length() - 1
    for k in range(codes.shape[0] // width):
        hot = []
        for j in range(width):
            line = codes[k * width + j : k * width + j + 1]
            hot.append(jnp.where(row_code == line, 1.0, 0.0).astype(bf16))
            low = jnp.where(low_code == (line & (share - 1)), 1.0, 0.0).astype(bf16)
            high = jnp.where(high_code == (line >> shift), 1.0, 0.0).astype(bf16)
            count = count + lax.dot_general(
                high, low, (((1,), (1,)), ((), ())), preferred_element_type=f32
            )
        part = jnp.dot(
            jnp.concatenate(hot, axis=1),
            act_ref[k * width * LANES : (k + 1) * width * LANES],
            preferred_element_type=f32,
        )
        if k == 0:
            acc_ref[...] = part
        else:
            acc_ref[...] += part
    cnt_ref[...] = count
    half = SHARDS // 2
    keep_ref[...] = acc_ref[: half * share].reshape(half, share, channels)
    for p in range(half):
        send_ref[p, :share] = acc_ref[(half + p) * share : (half + p + 1) * share].astype(bf16)
        send_ref[p, share:] = tail_rows(count[half + p : half + p + 1])


def quarter_kernel(keep_ref, cnt_ref, got_ref, mine_ref, mcnt_ref, s1_ref, s2_ref, s3_ref):
    share = keep_ref.shape[1]
    for p, out in enumerate((None, s1_ref, s2_ref, s3_ref)):
        value = keep_ref[p] + got_ref[p, :share].astype(f32)
        count = cnt_ref[p : p + 1] + untail(got_ref[p, share:])
        if out is None:
            mine_ref[...] = value
            mcnt_ref[...] = jnp.broadcast_to(count, (8, LANES))
        else:
            out[:share] = value.astype(bf16)
            out[share:] = tail_rows(count)


def gathered_kernel(mine_ref, mcnt_ref, a_ref, b_ref, c_ref, after_ref, out_ref):
    share = mine_ref.shape[0]
    value = mine_ref[...]
    count = mcnt_ref[0:1]
    for ref in (a_ref, b_ref, c_ref):
        value = value + ref[:share].astype(f32)
        count = count + untail(ref[share:])
    out_ref[:share] = value.astype(bf16)
    out_ref[share:] = tail_rows(count)


def pair_kernel(own_ref, got_ref, out_ref):
    share = own_ref.shape[0] - TAIL
    value = own_ref[:share].astype(f32) + got_ref[:share].astype(f32)
    out_ref[:share] = value.astype(bf16)
    out_ref[share:] = tail_rows(untail(own_ref[share:]) + untail(got_ref[share:]))


def project_kernel(own_ref, got_ref, w_ref, err_ref, out_ref):
    share = own_ref.shape[0] - TAIL
    value = own_ref[:share].astype(f32) + got_ref[:share].astype(f32)
    head = value.astype(bf16)
    rest = (value - head.astype(f32)).astype(bf16)
    sums = jnp.dot(head, w_ref[...], preferred_element_type=f32) + jnp.dot(
        rest, w_ref[...], preferred_element_type=f32
    )
    out_ref[:share] = sums.astype(bf16)
    out_ref[share:] = tail_rows(
        untail(own_ref[share:]) + untail(got_ref[share:]), err_ref[0:1]
    )


def as_column(row):
    return jnp.transpose(jnp.broadcast_to(row, (LANES, LANES)))


def latent_kernel(act_ref, w_ref, codes_ref, sum_ref, cnt_ref, after_ref, lat_ref, err_ref, head_ref, rest_ref):
    tokens, channels = lat_ref.shape
    codes_count = sum_ref.shape[0]
    clips = 2
    counts = cnt_ref[...]
    grand = jnp.sum(counts)
    smooth = (counts + smooth_eps) / (grand + codes_count * smooth_eps) * grand
    for i in range(codes_count // LANES):
        divisor = as_column(smooth[i : i + 1])
        divisor = jnp.concatenate([divisor] * (channels // LANES), axis=1)
        book = sum_ref[i * LANES : (i + 1) * LANES] / divisor
        head = book.astype(bf16)
        head_ref[i * LANES : (i + 1) * LANES] = head
        rest_ref[i * LANES : (i + 1) * LANES] = (book - head.astype(f32)).astype(bf16)
    lane_code = lax.broadcasted_iota(jnp.int32, (LANES, codes_count), 1)
    lane = lax.broadcasted_iota(jnp.int32, (1, LANES), 1)
    lines = tokens // LANES
    per_clip = lines // clips
    errors = jnp.zeros((1, LANES), f32)
    for c in range(clips):
        def step(i, acc):
            line = c * per_clip + i
            at = pl.ds(pl.multiple_of(line * LANES, LANES), LANES)
            latent = jnp.dot(act_ref[at], w_ref[...], preferred_element_type=f32)
            lat_ref[at] = latent
            column = as_column(codes_ref[pl.ds(line, 1)])
            column = jnp.concatenate([column] * (codes_count // LANES), axis=1)
            hot = jnp.where(column == lane_code, 1.0, 0.0).astype(bf16)
            chosen = jnp.dot(hot, head_ref[...], preferred_element_type=f32) + jnp.dot(
                hot, rest_ref[...], preferred_element_type=f32
            )
            away = latent - chosen
            away = away * away
            return acc + jnp.sum(away.reshape(LANES // 8, 8, channels), axis=0)

        total = lax.fori_loop(0, per_clip, step, jnp.zeros((8, channels), f32), unroll=True)
        errors = jnp.where(lane == c, jnp.sum(total), errors)
    err_ref[...] = jnp.broadcast_to(errors, (8, LANES))


def book_kernel(first, tokens, *refs):
    parts, (sum_ref, cnt_ref), rest = refs[:-8], refs[-8:-6], refs[-6:]
    _, _, book_hbm, count_ref, page_ref, sems = rest
    me = shard_bits()
    share = LANES
    channels = sum_ref.shape[1]
    grand = ema_decay * jnp.sum(cnt_ref[...]) + (1.0 - ema_decay) * tokens
    copies = []
    for i in range(SHARDS // 2):
        src = parts[i] if len(parts) > 1 else parts[0].at[i]
        shard = (first + i) ^ me
        count = ema_decay * cnt_ref[pl.ds(shard, 1)] + (1.0 - ema_decay) * untail(src[share:])
        count_ref[i : i + 1] = count
        smooth = (count + smooth_eps) / (grand + SHARDS * share * smooth_eps) * grand
        inverse = as_column(1.0 / smooth)
        inverse = jnp.concatenate([inverse] * (channels // LANES), axis=1)
        at = pl.ds(pl.multiple_of(shard * share, share), share)
        fresh = ema_decay * sum_ref[at] + (1.0 - ema_decay) * src[:share].astype(f32)
        page_ref[i] = fresh * inverse
        copies.append(pltpu.make_async_copy(page_ref.at[i], book_hbm.at[at], sems.at[i]))
        copies[-1].start()
    for copy in copies:
        copy.wait()


def early_kernel(tokens, p0, p1, p2, p3, sum_ref, cnt_ref, book_hbm, count_ref, page_ref, sems):
    book_kernel(0, tokens, p0, p1, p2, p3, sum_ref, cnt_ref, None, None, book_hbm, count_ref, page_ref, sems)


def late_kernel(tokens, q_ref, sum_ref, cnt_ref, book_in, early_ref, book_hbm, count_ref, page_ref, late_ref, sems):
    book_kernel(
        SHARDS // 2, tokens, q_ref, sum_ref, cnt_ref, None, None, book_hbm, late_ref, page_ref, sems
    )
    me = shard_bits()
    for i in range(SHARDS // 2):
        count_ref[pl.ds(i ^ me, 1)] = early_ref[i : i + 1]
        count_ref[pl.ds((SHARDS // 2 + i) ^ me, 1)] = late_ref[i : i + 1]


def error_kernel(scale, p1, err_ref, error_ref):
    error_ref[...] = jnp.broadcast_to(
        (err_ref[0:1] + untail(p1[LANES:], 1)) * scale, (8, LANES)
    )


def body(video, gain_first, conv_weight, gain_second, proj_weight, codes, ema_sum, ema_count):
    clips, frames, rows, cols, channels = video.shape
    codes_count = ema_sum.shape[0]
    clip_size, strips = lax.axis_size("clip"), lax.axis_size("strip")
    n = clip_size * strips
    share = codes_count // SHARDS
    assert strips == 2 and clip_size >= 4 and clip_size & (clip_size - 1) == 0
    assert share == LANES and channels == 2 * LANES and clips == 2

    def swap(x, mask):
        return lax.ppermute(x, BOTH, [(i, i ^ mask) for i in range(n)])

    tokens = frames * rows * cols
    halo = clips * frames * cols
    pay, near, held, taps = call(
        stats_kernel,
        [
            ((halo + 16, channels), bf16),
            ((16, channels), f32),
            (video.shape, bf16),
            ((min(3, frames), 9 * channels, channels), bf16),
        ],
        [pltpu.with_memory_space_constraint(video, pltpu.HBM), pltpu.with_memory_space_constraint(conv_weight.reshape(3, 9 * channels, channels), pltpu.HBM)],
        scratch=[pltpu.SemaphoreType.DMA((clips + 1,))],
        flops=10_000_000,
        limit=16 << 20,
        name="stats",
        far=(0, 1),
    )
    far_pay = swap(pay, 1)
    code_lines = codes.reshape(-1, LANES)
    hidden, near_two = call(
        conv_kernel,
        [((clips, tokens, channels), f32), ((16, channels), f32)],
        [held, far_pay, near, gain_first.reshape(1, channels), taps],
        scratch=[VMEM((clips, frames, rows + 2, cols, 3 * channels), bf16)],
        flops=4_000_000_000,
        limit=24 << 20,
        name="conv",
    )
    far_two = swap(near_two, 1)
    act, send, keep, cnt = call(
        segment_kernel,
        [
            ((clips * tokens, channels), bf16),
            ((SHARDS // 2, share + TAIL, channels), bf16),
            ((SHARDS // 2, share, channels), f32),
            ((SHARDS, LANES), f32),
        ],
        [hidden, near_two, far_two, gain_second.reshape(1, channels), code_lines],
        scratch=[VMEM((codes_count, channels), f32)],
        flops=1_500_000_000,
        limit=24 << 20,
        name="segment",
    )
    core, x_bit = 2, 4
    got = swap(send, core)
    counts = ema_count.reshape(SHARDS, LANES)
    flat = ((share + TAIL, channels), bf16)
    mine, mine_cnt, s1, s2, s3 = call(
        quarter_kernel,
        [((share, channels), f32), ((8, LANES), f32), flat, flat, flat],
        [keep, cnt, got],
        flops=1_000_000,
        limit=8 << 20,
        name="quarter",
    )
    near_masks = (1, x_bit, 1 | x_bit)
    parts = [swap(s, m) for s, m in zip((s1, s2, s3), near_masks)]
    latent, err = call(
        latent_kernel,
        [((clips * tokens, channels), f32), ((8, LANES), f32)],
        [act, proj_weight, code_lines, ema_sum, counts, mine_cnt],
        scratch=[VMEM((codes_count, channels), bf16)] * 2,
        flops=2_500_000_000,
        limit=24 << 20,
        name="latent",
    )
    (own,) = call(
        gathered_kernel, [flat], [mine, mine_cnt, *parts, err], flops=1_000_000, limit=8 << 20, name="gathered"
    )
    bit = 8
    while bit < n // 2:
        (own,) = call(
            pair_kernel, [flat], [own, swap(own, bit)], flops=1_000_000, limit=8 << 20, name="pair"
        )
        bit *= 2
    last = swap(own, bit) if bit < n else jnp.zeros_like(own)
    (done,) = call(
        project_kernel, [flat], [own, last, proj_weight, err], flops=1_000_000, limit=8 << 20, name="project"
    )
    peers = [swap(done, m) for m in near_masks]
    across = swap(jnp.stack([done, *peers]), core)
    scale = 1.0 / (tokens * strips * channels)
    total_tokens = float(clips * tokens * n)
    half = SHARDS // 2
    (error,) = call(
        functools.partial(error_kernel, scale),
        [((8, LANES), f32)],
        [peers[0], err],
        flops=1_000_000,
        limit=8 << 20,
        name="error",
    )
    page = VMEM((half, share, channels), f32)
    book_shape = ((codes_count, channels), f32)
    book, early = call(
        functools.partial(early_kernel, total_tokens),
        [book_shape, ((8, LANES), f32)],
        [done, *peers, ema_sum, counts],
        scratch=[page, pltpu.SemaphoreType.DMA((half,))],
        flops=1_000_000,
        limit=8 << 20,
        name="early",
        far_outs=(0,),
    )
    book, count = call(
        functools.partial(late_kernel, total_tokens),
        [book_shape, ((SHARDS, LANES), f32)],
        [across, ema_sum, counts, book, early],
        scratch=[page, VMEM((8, LANES), f32), pltpu.SemaphoreType.DMA((half,))],
        flops=1_000_000,
        limit=8 << 20,
        name="late",
        far=(3,),
        far_outs=(0,),
        alias={3: 0},
    )
    return (
        latent.reshape(clips, frames, rows, cols, channels),
        book,
        count.reshape(codes_count),
        error[0, :clips],
    )


def solution(mesh):
    in_specs = (
        P("clip", None, "strip", None, None),
        P(),
        P(),
        P(),
        P(),
        P("clip", None, "strip", None),
        P(),
        P(),
    )
    out_specs = (P("clip", None, "strip", None, None), P(), P(), P("clip"))
    return jax.shard_map(body, mesh=mesh, in_specs=in_specs, out_specs=out_specs, check_vma=False)
```

```python
import functools

import jax
import jax.numpy as jnp
from jax import lax
from jax.experimental import pallas as pl
from jax.experimental.pallas import tpu as pltpu
from jax.sharding import PartitionSpec as P

GROUPS = 32

norm_eps = 1e-06
smooth_eps = 1e-05
ema_decay = 0.9

f32 = jnp.float32
bf16 = jnp.bfloat16
LANES = 128
SHARDS = 8
TAIL = 8
BOTH = ("clip", "strip")
VMEM = pltpu.VMEM
VSPEC = pl.BlockSpec(memory_space=pltpu.VMEM)


def call(kernel, outs, args, scratch=(), flops=0, limit=None, name=None, far=(), far_outs=(), alias=None):
    far_spec = pl.BlockSpec(memory_space=pltpu.HBM)
    return pl.pallas_call(
        kernel,
        out_shape=tuple(jax.ShapeDtypeStruct(s, d) for s, d in outs),
        in_specs=[far_spec if i in far else VSPEC for i in range(len(args))],
        out_specs=tuple(far_spec if i in far_outs else VSPEC for i in range(len(outs))),
        scratch_shapes=list(scratch),
        input_output_aliases=alias or {},
        compiler_params=pltpu.CompilerParams(vmem_limit_bytes=limit),
        cost_estimate=pl.CostEstimate(flops=flops, bytes_accessed=0, transcendentals=0),
        name=name,
    )(*args)


def pieces(value):
    head = value.astype(bf16)
    rest = value - head.astype(f32)
    middle = rest.astype(bf16)
    last = (rest - middle.astype(f32)).astype(bf16)
    return head, middle, last


def group_matrix(channels):
    shift = (channels // GROUPS).bit_length() - 1
    rows = lax.broadcasted_iota(jnp.int32, (channels, channels), 0) >> shift
    cols = lax.broadcasted_iota(jnp.int32, (channels, channels), 1) >> shift
    return jnp.where(rows == cols, 1.0, 0.0).astype(bf16)


def group_total(rows, matrix):
    split = [p.astype(f32) for p in pieces(rows)]
    split = jnp.concatenate(split + [jnp.zeros_like(rows)], axis=0).astype(bf16)
    total = jnp.dot(split, matrix, preferred_element_type=f32)
    return total[0:8] + total[8:16] + total[16:24]


def stacked(rows, channels):
    row = lax.broadcasted_iota(jnp.int32, (8, channels), 0)
    out = jnp.zeros((8, channels), f32)
    for i, value in enumerate(rows):
        out = jnp.where(row == i, value, out)
    return out


def local_stats(read, clips, blocks, rows, channels, ready=lambda c: None):
    matrix = group_matrix(channels)
    members = blocks * rows * (channels // GROUPS)

    def over(c, term):
        parts = [None] * 2
        for i in range(blocks):
            value = term(read(c, i))
            parts[i % 2] = value if parts[i % 2] is None else parts[i % 2] + value
        total = parts[0] if parts[1] is None else parts[0] + parts[1]
        return jnp.sum(total, axis=0, keepdims=True)

    sums = []
    for c in range(clips):
        ready(c)
        sums.append(over(c, lambda x: x))
    means = group_total(stacked(sums, channels), matrix) / members

    def squared(c):
        mean = means[c : c + 1]

        def term(x):
            away = x - mean
            return away * away

        return over(c, term)

    squares = group_total(stacked([squared(c) for c in range(clips)], channels), matrix)
    return means, squares


def merged(mean_a, square_a, mean_b, square_b, members):
    mean = 0.5 * (mean_a + mean_b)
    apart = mean_a - mean_b
    spread = (square_a + square_b + apart * apart * (0.5 * members)) / (2 * members)
    return mean, lax.rsqrt(spread + norm_eps)


def silu(v):
    half = 0.5 * v
    return half + half * jnp.tanh(half)


def stats_kernel(video_hbm, w_hbm, pay_ref, loc_ref, video_ref, w_ref, sems):
    clips, frames, rows, cols, channels = video_ref.shape
    strip = lax.axis_index("strip")
    loads = [
        pltpu.make_async_copy(video_hbm.at[c], video_ref.at[c], sems.at[c]) for c in range(clips)
    ]
    first_tap = w_hbm.shape[0] - w_ref.shape[0]
    taps = pltpu.make_async_copy(w_hbm.at[pl.ds(first_tap, w_ref.shape[0])], w_ref, sems.at[clips])
    for load in loads:
        load.start()
    taps.start()

    def read(c, i):
        return video_ref[c, i // rows, i % rows].astype(f32)

    means, squares = local_stats(
        read, clips, frames * rows, cols, channels, ready=lambda c: loads[c].wait()
    )
    edge = (1 - strip) * (rows - 1)
    for c in range(clips):
        for t in range(frames):
            at = (c * frames + t) * cols
            pay_ref[at : at + cols] = video_ref[c, t, edge]

    loc_ref[0:8] = means
    loc_ref[8:16] = squares
    base = clips * frames * cols
    row = lax.broadcasted_iota(jnp.int32, (16, channels), 0)
    out = jnp.zeros((16, channels), f32)
    for j, value in enumerate((means, squares)):
        for k, piece in enumerate(pieces(value)):
            piece = piece.astype(f32)
            for c in range(clips):
                out = jnp.where(row == (j * clips + c) * 3 + k, piece[c : c + 1], out)
    pay_ref[base : base + 16] = out.astype(bf16)
    taps.wait()


def conv_kernel(video_ref, pay_ref, loc_ref, gain_ref, w_ref, hid_ref, st_ref, buf_ref):
    clips, frames, rows, cols, channels = video_ref.shape
    strip = lax.axis_index("strip")
    members = frames * rows * cols * (channels // GROUPS)
    base = clips * frames * cols
    first_tap = 3 - w_ref.shape[0]
    far = pay_ref[base : base + 16].astype(f32)
    gain = gain_ref[...]
    col = lax.broadcasted_iota(jnp.int32, (cols, channels), 0)

    def put(c, t, r, act):
        left = jnp.where(col == 0, 0.0, pltpu.roll(act, 1, 0))
        right = jnp.where(col == cols - 1, 0.0, pltpu.roll(act, cols - 1, 0))
        buf_ref[c, t, r, :, 0:channels] = left.astype(bf16)
        buf_ref[c, t, r, :, channels : 2 * channels] = act.astype(bf16)
        buf_ref[c, t, r, :, 2 * channels : 3 * channels] = right.astype(bf16)

    for c in range(clips):
        at = [(j * clips + c) * 3 for j in (0, 1)]
        far_mean, far_square = [far[i : i + 1] + far[i + 1 : i + 2] + far[i + 2 : i + 3] for i in at]
        mean, inverse = merged(
            loc_ref[c : c + 1], loc_ref[8 + c : 9 + c], far_mean, far_square, members
        )
        scale = inverse * gain
        for t in range(frames):
            def row_step(r, carry):
                x = video_ref[c, t, r].astype(f32)
                put(c, t, r + 1, silu((x - mean) * scale))
                return carry

            lax.fori_loop(0, rows, row_step, 0, unroll=True)
            where_at = (c * frames + t) * cols
            halo = silu((pay_ref[where_at : where_at + cols].astype(f32) - mean) * scale)
            put(c, t, 0, jnp.where(strip > 0, halo, 0.0))
            put(c, t, rows + 1, jnp.where(strip > 0, 0.0, halo))

        def patches(t):
            return jnp.concatenate(
                [
                    buf_ref[c, t, b : b + rows].reshape(rows * cols, 3 * channels)
                    for b in range(3)
                ],
                axis=1,
            )

        for t in range(frames):
            total = video_ref[c, t].reshape(rows * cols, channels).astype(f32)
            for a in range(3):
                if t + a - 2 >= 0:
                    total = total + jnp.dot(
                        patches(t + a - 2), w_ref[a - first_tap], preferred_element_type=f32
                    )
            hid_ref[c, t * rows * cols : (t + 1) * rows * cols] = total

    def read(c, i):
        return hid_ref[c, i * cols : (i + 1) * cols]

    means, squares = local_stats(read, clips, frames * rows, cols, channels)
    st_ref[...] = stacked(
        [m[c : c + 1] for m in (means, squares) for c in range(clips)], channels
    )


def shard_bits():
    clip = lax.axis_index("clip")
    return ((clip & 1) << 2) | (((clip >> 1) & 1) << 1) | lax.axis_index("strip")


def tail_rows(count, extra=None):
    row = lax.broadcasted_iota(jnp.int32, (TAIL, 2 * LANES), 0)
    zero = jnp.zeros((1, LANES), f32)
    out = jnp.zeros((TAIL, 2 * LANES), f32)
    for i, value in enumerate((count,) if extra is None else (count, extra)):
        head, middle, last = [p.astype(f32) for p in pieces(value)]
        out = jnp.where(row == 2 * i, jnp.concatenate([head, middle], axis=1), out)
        out = jnp.where(row == 2 * i + 1, jnp.concatenate([last, zero], axis=1), out)
    return out.astype(bf16)


def untail(block, which=0):
    block = block.astype(f32)
    i = 2 * which
    return (
        block[i : i + 1, :LANES] + block[i : i + 1, LANES:] + block[i + 1 : i + 2, :LANES]
    )


def hot_rows(codes_ref, act_ref, acc_ref, first):
    share = LANES
    rows = acc_ref.shape[0]
    codes = codes_ref[...] ^ (shard_bits() * share)
    row_code = lax.broadcasted_iota(jnp.int32, (rows, LANES), 0) + first * share
    width = 2
    for k in range(codes.shape[0] // width):
        hot = []
        for j in range(width):
            line = codes[k * width + j : k * width + j + 1]
            hot.append(jnp.where(row_code == line, 1.0, 0.0).astype(bf16))
        part = jnp.dot(
            jnp.concatenate(hot, axis=1),
            act_ref[k * width * LANES : (k + 1) * width * LANES],
            preferred_element_type=f32,
        )
        if k == 0:
            acc_ref[...] = part
        else:
            acc_ref[...] += part


def segment_kernel(
    hid_ref, near_ref, far_ref, gain_ref, codes_ref, act_ref, send_ref, cnt_ref, acc_ref
):
    clips, tokens, channels = hid_ref.shape
    members = tokens * (channels // GROUPS)
    gain = gain_ref[...]
    block = 64
    for c in range(clips):
        mean, inverse = merged(
            near_ref[c : c + 1],
            near_ref[clips + c : clips + c + 1],
            far_ref[c : c + 1],
            far_ref[clips + c : clips + c + 1],
            members,
        )
        scale = inverse * gain
        for i in range(tokens // block):
            x = hid_ref[c, i * block : (i + 1) * block]
            act = silu((x - mean) * scale).astype(bf16)
            act_ref[c * tokens + i * block : c * tokens + (i + 1) * block] = act

    share = LANES
    half = SHARDS // 2
    codes = codes_ref[...] ^ (shard_bits() * share)
    low_code = lax.broadcasted_iota(jnp.int32, (share, LANES), 0)
    high_code = lax.broadcasted_iota(jnp.int32, (SHARDS, LANES), 0)
    count = jnp.zeros((SHARDS, LANES), f32)
    shift = share.bit_length() - 1
    for k in range(codes.shape[0]):
        line = codes[k : k + 1]
        low = jnp.where(low_code == (line & (share - 1)), 1.0, 0.0).astype(bf16)
        high = jnp.where(high_code == (line >> shift), 1.0, 0.0).astype(bf16)
        count = count + lax.dot_general(
            high, low, (((1,), (1,)), ((), ())), preferred_element_type=f32
        )
    cnt_ref[...] = count
    hot_rows(codes_ref, act_ref, acc_ref, half)
    for p in range(half):
        send_ref[p, :share] = acc_ref[p * share : (p + 1) * share].astype(bf16)
        send_ref[p, share:] = tail_rows(count[half + p : half + p + 1])


def keep_kernel(act_ref, codes_ref, keep_ref):
    hot_rows(codes_ref, act_ref, keep_ref, 0)


def quarter_kernel(keep_ref, cnt_ref, got_ref, mine_ref, mcnt_ref, s1_ref, s2_ref, s3_ref):
    share = LANES
    for p, out in enumerate((None, s1_ref, s2_ref, s3_ref)):
        value = keep_ref[p * share : (p + 1) * share] + got_ref[p, :share].astype(f32)
        count = cnt_ref[p : p + 1] + untail(got_ref[p, share:])
        if out is None:
            mine_ref[...] = value
            mcnt_ref[...] = jnp.broadcast_to(count, (8, LANES))
        else:
            out[:share] = value.astype(bf16)
            out[share:] = tail_rows(count)


def gathered_kernel(mine_ref, mcnt_ref, a_ref, b_ref, c_ref, after_ref, out_ref):
    share = mine_ref.shape[0]
    value = mine_ref[...]
    count = mcnt_ref[0:1]
    for ref in (a_ref, b_ref, c_ref):
        value = value + ref[:share].astype(f32)
        count = count + untail(ref[share:])
    out_ref[:share] = value.astype(bf16)
    out_ref[share:] = tail_rows(count)


def pair_kernel(own_ref, got_ref, out_ref):
    share = own_ref.shape[0] - TAIL
    value = own_ref[:share].astype(f32) + got_ref[:share].astype(f32)
    out_ref[:share] = value.astype(bf16)
    out_ref[share:] = tail_rows(untail(own_ref[share:]) + untail(got_ref[share:]))


def project_kernel(own_ref, got_ref, w_ref, err_ref, out_ref):
    share = own_ref.shape[0] - TAIL
    value = own_ref[:share].astype(f32) + got_ref[:share].astype(f32)
    head = value.astype(bf16)
    rest = (value - head.astype(f32)).astype(bf16)
    sums = jnp.dot(head, w_ref[...], preferred_element_type=f32) + jnp.dot(
        rest, w_ref[...], preferred_element_type=f32
    )
    out_ref[:share] = sums.astype(bf16)
    out_ref[share:] = tail_rows(
        untail(own_ref[share:]) + untail(got_ref[share:]), err_ref[0:1]
    )


def as_column(row):
    return jnp.transpose(jnp.broadcast_to(row, (LANES, LANES)))


def latent_kernel(act_ref, w_ref, codes_ref, sum_ref, cnt_ref, after_ref, lat_ref, err_ref, head_ref, rest_ref):
    tokens, channels = lat_ref.shape
    codes_count = sum_ref.shape[0]
    clips = 2
    counts = cnt_ref[...]
    grand = jnp.sum(counts)
    smooth = (counts + smooth_eps) / (grand + codes_count * smooth_eps) * grand
    for i in range(codes_count // LANES):
        divisor = as_column(smooth[i : i + 1])
        divisor = jnp.concatenate([divisor] * (channels // LANES), axis=1)
        book = sum_ref[i * LANES : (i + 1) * LANES] / divisor
        head = book.astype(bf16)
        head_ref[i * LANES : (i + 1) * LANES] = head
        rest_ref[i * LANES : (i + 1) * LANES] = (book - head.astype(f32)).astype(bf16)
    lane_code = lax.broadcasted_iota(jnp.int32, (LANES, codes_count), 1)
    lane = lax.broadcasted_iota(jnp.int32, (1, LANES), 1)
    lines = tokens // LANES
    per_clip = lines // clips
    errors = jnp.zeros((1, LANES), f32)
    for c in range(clips):
        def step(i, acc):
            line = c * per_clip + i
            at = pl.ds(pl.multiple_of(line * LANES, LANES), LANES)
            latent = jnp.dot(act_ref[at], w_ref[...], preferred_element_type=f32)
            lat_ref[at] = latent
            column = as_column(codes_ref[pl.ds(line, 1)])
            column = jnp.concatenate([column] * (codes_count // LANES), axis=1)
            hot = jnp.where(column == lane_code, 1.0, 0.0).astype(bf16)
            chosen = jnp.dot(hot, head_ref[...], preferred_element_type=f32) + jnp.dot(
                hot, rest_ref[...], preferred_element_type=f32
            )
            away = latent - chosen
            away = away * away
            return acc + jnp.sum(away.reshape(LANES // 8, 8, channels), axis=0)

        total = lax.fori_loop(0, per_clip, step, jnp.zeros((8, channels), f32), unroll=True)
        errors = jnp.where(lane == c, jnp.sum(total), errors)
    err_ref[...] = jnp.broadcast_to(errors, (8, LANES))


def book_kernel(first, tokens, *refs, done=lambda: None):
    parts, (sum_ref, cnt_ref), rest = refs[:-8], refs[-8:-6], refs[-6:]
    _, _, book_hbm, count_ref, page_ref, sems = rest
    me = shard_bits()
    share = LANES
    channels = sum_ref.shape[1]
    grand = ema_decay * jnp.sum(cnt_ref[...]) + (1.0 - ema_decay) * tokens
    copies = []
    for i in range(SHARDS // 2):
        src = parts[i] if len(parts) > 1 else parts[0].at[i]
        shard = (first + i) ^ me
        count = ema_decay * cnt_ref[pl.ds(shard, 1)] + (1.0 - ema_decay) * untail(src[share:])
        count_ref[i : i + 1] = count
        smooth = (count + smooth_eps) / (grand + SHARDS * share * smooth_eps) * grand
        inverse = as_column(1.0 / smooth)
        inverse = jnp.concatenate([inverse] * (channels // LANES), axis=1)
        at = pl.ds(pl.multiple_of(shard * share, share), share)
        fresh = ema_decay * sum_ref[at] + (1.0 - ema_decay) * src[:share].astype(f32)
        page_ref[i] = fresh * inverse
        copies.append(pltpu.make_async_copy(page_ref.at[i], book_hbm.at[at], sems.at[i]))
        copies[-1].start()
    done()
    for copy in copies:
        copy.wait()


def early_kernel(tokens, p0, p1, p2, p3, sum_ref, cnt_ref, book_hbm, count_ref, page_ref, sems):
    book_kernel(0, tokens, p0, p1, p2, p3, sum_ref, cnt_ref, None, None, book_hbm, count_ref, page_ref, sems)


def late_kernel(tokens, q_ref, sum_ref, cnt_ref, book_in, early_ref, book_hbm, count_hbm, page_ref, late_ref, line_ref, sems):
    half = SHARDS // 2
    copy = pltpu.make_async_copy(line_ref, count_hbm, sems.at[half])

    def counts():
        me = shard_bits()
        for i in range(half):
            line_ref[pl.ds(i ^ me, 1)] = early_ref[i : i + 1]
            line_ref[pl.ds((half + i) ^ me, 1)] = late_ref[i : i + 1]
        copy.start()

    book_kernel(
        half, tokens, q_ref, sum_ref, cnt_ref, None, None, book_hbm, late_ref, page_ref, sems, done=counts
    )
    copy.wait()


def error_kernel(scale, p1, err_ref, error_ref):
    error_ref[...] = jnp.broadcast_to(
        (err_ref[0:1] + untail(p1[LANES:], 1)) * scale, (8, LANES)
    )


def body(video, gain_first, conv_weight, gain_second, proj_weight, codes, ema_sum, ema_count):
    clips, frames, rows, cols, channels = video.shape
    codes_count = ema_sum.shape[0]
    clip_size, strips = lax.axis_size("clip"), lax.axis_size("strip")
    n = clip_size * strips
    share = codes_count // SHARDS
    assert strips == 2 and clip_size >= 4 and clip_size & (clip_size - 1) == 0
    assert share == LANES and channels == 2 * LANES and clips == 2

    def swap(x, mask):
        return lax.ppermute(x, BOTH, [(i, i ^ mask) for i in range(n)])

    tokens = frames * rows * cols
    halo = clips * frames * cols
    pay, near, held, taps = call(
        stats_kernel,
        [
            ((halo + 16, channels), bf16),
            ((16, channels), f32),
            (video.shape, bf16),
            ((min(3, frames), 9 * channels, channels), bf16),
        ],
        [pltpu.with_memory_space_constraint(video, pltpu.HBM), pltpu.with_memory_space_constraint(conv_weight.reshape(3, 9 * channels, channels), pltpu.HBM)],
        scratch=[pltpu.SemaphoreType.DMA((clips + 1,))],
        flops=10_000_000,
        limit=16 << 20,
        name="stats",
        far=(0, 1),
    )
    far_pay = swap(pay, 1)
    code_lines = codes.reshape(-1, LANES)
    hidden, near_two = call(
        conv_kernel,
        [((clips, tokens, channels), f32), ((8, channels), f32)],
        [held, far_pay, near, gain_first.reshape(1, channels), taps],
        scratch=[VMEM((clips, frames, rows + 2, cols, 3 * channels), bf16)],
        flops=4_000_000_000,
        limit=24 << 20,
        name="conv",
    )
    far_two = swap(near_two, 1)
    act, send, cnt = call(
        segment_kernel,
        [
            ((clips * tokens, channels), bf16),
            ((SHARDS // 2, share + TAIL, channels), bf16),
            ((SHARDS, LANES), f32),
        ],
        [hidden, near_two, far_two, gain_second.reshape(1, channels), code_lines],
        scratch=[VMEM((codes_count // 2, channels), f32)],
        flops=1_500_000_000,
        limit=24 << 20,
        name="segment",
    )
    core, x_bit = 2, 4
    got = swap(send, core)
    (keep,) = call(
        keep_kernel,
        [((codes_count // 2, channels), f32)],
        [act, code_lines],
        flops=1_000_000_000,
        limit=8 << 20,
        name="keep",
    )
    counts = ema_count.reshape(SHARDS, LANES)
    flat = ((share + TAIL, channels), bf16)
    mine, mine_cnt, s1, s2, s3 = call(
        quarter_kernel,
        [((share, channels), f32), ((8, LANES), f32), flat, flat, flat],
        [keep, cnt, got],
        flops=1_000_000,
        limit=8 << 20,
        name="quarter",
    )
    near_masks = (1, x_bit, 1 | x_bit)
    parts = [swap(s, m) for s, m in zip((s1, s2, s3), near_masks)]
    latent, err = call(
        latent_kernel,
        [((clips * tokens, channels), f32), ((8, LANES), f32)],
        [act, proj_weight, code_lines, ema_sum, counts, mine_cnt],
        scratch=[VMEM((codes_count, channels), bf16)] * 2,
        flops=2_500_000_000,
        limit=24 << 20,
        name="latent",
    )
    (own,) = call(
        gathered_kernel, [flat], [mine, mine_cnt, *parts, err], flops=1_000_000, limit=8 << 20, name="gathered"
    )
    bit = 8
    while bit < n // 2:
        (own,) = call(
            pair_kernel, [flat], [own, swap(own, bit)], flops=1_000_000, limit=8 << 20, name="pair"
        )
        bit *= 2
    last = swap(own, bit) if bit < n else jnp.zeros_like(own)
    (done,) = call(
        project_kernel, [flat], [own, last, proj_weight, err], flops=1_000_000, limit=8 << 20, name="project"
    )
    peers = [swap(done, m) for m in near_masks]
    across = swap(jnp.stack([done, *peers]), core)
    scale = 1.0 / (tokens * strips * channels)
    total_tokens = float(clips * tokens * n)
    half = SHARDS // 2
    (error,) = call(
        functools.partial(error_kernel, scale),
        [((8, LANES), f32)],
        [peers[0], err],
        flops=1_000_000,
        limit=8 << 20,
        name="error",
    )
    page = VMEM((half, share, channels), f32)
    book_shape = ((codes_count, channels), f32)
    book, early = call(
        functools.partial(early_kernel, total_tokens),
        [book_shape, ((8, LANES), f32)],
        [done, *peers, ema_sum, counts],
        scratch=[page, pltpu.SemaphoreType.DMA((half,))],
        flops=1_000_000,
        limit=8 << 20,
        name="early",
        far_outs=(0,),
    )
    book, count = call(
        functools.partial(late_kernel, total_tokens),
        [book_shape, ((SHARDS, LANES), f32)],
        [across, ema_sum, counts, book, early],
        scratch=[
            page,
            VMEM((8, LANES), f32),
            VMEM((SHARDS, LANES), f32),
            pltpu.SemaphoreType.DMA((half + 1,)),
        ],
        flops=1_000_000,
        limit=8 << 20,
        name="late",
        far=(3,),
        far_outs=(0, 1),
        alias={3: 0},
    )
    return (
        latent.reshape(clips, frames, rows, cols, channels),
        book,
        count.reshape(codes_count),
        error[0, :clips],
    )


def solution(mesh):
    in_specs = (
        P("clip", None, "strip", None, None),
        P(),
        P(),
        P(),
        P(),
        P("clip", None, "strip", None),
        P(),
        P(),
    )
    out_specs = (P("clip", None, "strip", None, None), P(), P(), P("clip"))
    return jax.shard_map(body, mesh=mesh, in_specs=in_specs, out_specs=out_specs, check_vma=False)
```

```python
import functools

import jax
import jax.numpy as jnp
from jax import lax
from jax.experimental import pallas as pl
from jax.experimental.pallas import tpu as pltpu
from jax.sharding import PartitionSpec as P

GROUPS = 32

norm_eps = 1e-06
smooth_eps = 1e-05
ema_decay = 0.9

f32 = jnp.float32
bf16 = jnp.bfloat16
LANES = 128
SHARDS = 8
TAIL = 8
BOTH = ("clip", "strip")
VMEM = pltpu.VMEM
VSPEC = pl.BlockSpec(memory_space=pltpu.VMEM)


def call(kernel, outs, args, scratch=(), flops=0, limit=None, name=None, far=(), far_outs=(), alias=None):
    far_spec = pl.BlockSpec(memory_space=pltpu.HBM)
    return pl.pallas_call(
        kernel,
        out_shape=tuple(jax.ShapeDtypeStruct(s, d) for s, d in outs),
        in_specs=[far_spec if i in far else VSPEC for i in range(len(args))],
        out_specs=tuple(far_spec if i in far_outs else VSPEC for i in range(len(outs))),
        scratch_shapes=list(scratch),
        input_output_aliases=alias or {},
        compiler_params=pltpu.CompilerParams(vmem_limit_bytes=limit),
        cost_estimate=pl.CostEstimate(flops=flops, bytes_accessed=0, transcendentals=0),
        name=name,
    )(*args)


def pieces(value):
    head = value.astype(bf16)
    rest = value - head.astype(f32)
    middle = rest.astype(bf16)
    last = (rest - middle.astype(f32)).astype(bf16)
    return head, middle, last


def group_matrix(channels):
    shift = (channels // GROUPS).bit_length() - 1
    rows = lax.broadcasted_iota(jnp.int32, (channels, channels), 0) >> shift
    cols = lax.broadcasted_iota(jnp.int32, (channels, channels), 1) >> shift
    return jnp.where(rows == cols, 1.0, 0.0).astype(bf16)


def group_total(rows, matrix):
    split = [p.astype(f32) for p in pieces(rows)]
    split = jnp.concatenate(split + [jnp.zeros_like(rows)], axis=0).astype(bf16)
    total = jnp.dot(split, matrix, preferred_element_type=f32)
    return total[0:8] + total[8:16] + total[16:24]


def stacked(rows, channels):
    row = lax.broadcasted_iota(jnp.int32, (8, channels), 0)
    out = jnp.zeros((8, channels), f32)
    for i, value in enumerate(rows):
        out = jnp.where(row == i, value, out)
    return out


def local_stats(read, clips, blocks, rows, channels, ready=lambda c: None):
    matrix = group_matrix(channels)
    members = blocks * rows * (channels // GROUPS)
    some = max(1, blocks // 8)

    def over(c, count, *terms):
        totals = []
        for term in terms:
            parts = [None] * 2
            for i in range(count):
                value = term(read(c, i))
                parts[i % 2] = value if parts[i % 2] is None else parts[i % 2] + value
            total = parts[0] if parts[1] is None else parts[0] + parts[1]
            totals.append(jnp.sum(total, axis=0, keepdims=True))
        return totals

    count = blocks * rows
    points, near, squares = [], [], []
    passes = []
    for c in range(clips):
        ready(c)
        point = over(c, some, lambda x: x)[0] * (1.0 / (some * rows))
        points.append(point)
        passes.append(over(c, blocks, lambda x: x - point, lambda x: (x - point) * (x - point)))
    pivot = group_total(stacked(points, channels), matrix) * (count / members)
    for c in range(clips):
        point = points[c]
        total, square = passes[c]
        apart = point - pivot[c : c + 1]
        near.append(total + count * apart)
        squares.append(square + 2.0 * apart * total + count * apart * apart)
    sums = near
    totals = group_total(stacked(sums + squares, channels), matrix)
    offset = totals[0:clips] / members
    square = jnp.maximum(totals[clips : 2 * clips] - totals[0:clips] * offset, 0.0)
    return pivot[0:clips] + offset, square


def merged(mean_a, square_a, mean_b, square_b, members):
    mean = 0.5 * (mean_a + mean_b)
    apart = mean_a - mean_b
    spread = (square_a + square_b + apart * apart * (0.5 * members)) / (2 * members)
    return mean, lax.rsqrt(spread + norm_eps)


def silu(v):
    half = 0.5 * v
    return half + half * jnp.tanh(half)


def taps_kernel(w_hbm, after_ref, w_ref, sem):
    first_tap = w_hbm.shape[0] - w_ref.shape[0]
    load = pltpu.make_async_copy(w_hbm.at[pl.ds(first_tap, w_ref.shape[0])], w_ref, sem.at[0])
    load.start()
    load.wait()


def stats_kernel(video_hbm, pay_ref, loc_ref, video_ref, sems):
    clips, frames, rows, cols, channels = video_ref.shape
    strip = lax.axis_index("strip")
    loads = [
        pltpu.make_async_copy(video_hbm.at[c], video_ref.at[c], sems.at[c]) for c in range(clips)
    ]
    for load in loads:
        load.start()

    def read(c, i):
        return video_ref[c, i // rows, i % rows].astype(f32)

    means, squares = local_stats(
        read, clips, frames * rows, cols, channels, ready=lambda c: loads[c].wait()
    )
    edge = (1 - strip) * (rows - 1)
    for c in range(clips):
        for t in range(frames):
            at = (c * frames + t) * cols
            pay_ref[at : at + cols] = video_ref[c, t, edge]

    loc_ref[...] = stacked([m[c : c + 1] for m in (means, squares) for c in range(clips)], channels)
    base = clips * frames * cols
    row = lax.broadcasted_iota(jnp.int32, (16, channels), 0)
    out = jnp.zeros((16, channels), f32)
    for j, value in enumerate((means, squares)):
        for k, piece in enumerate(pieces(value)):
            piece = piece.astype(f32)
            for c in range(clips):
                out = jnp.where(row == (j * clips + c) * 3 + k, piece[c : c + 1], out)
    pay_ref[base : base + 16] = out.astype(bf16)


def conv_kernel(video_ref, pay_ref, loc_ref, gain_ref, w_ref, hid_ref, st_ref, buf_ref):
    clips, frames, rows, cols, channels = video_ref.shape
    strip = lax.axis_index("strip")
    members = frames * rows * cols * (channels // GROUPS)
    base = clips * frames * cols
    first_tap = 3 - w_ref.shape[0]
    far = pay_ref[base : base + 16].astype(f32)
    gain = gain_ref[...]
    col = lax.broadcasted_iota(jnp.int32, (cols, channels), 0)

    def put(c, t, r, act):
        left = jnp.where(col == 0, 0.0, pltpu.roll(act, 1, 0))
        right = jnp.where(col == cols - 1, 0.0, pltpu.roll(act, cols - 1, 0))
        buf_ref[c, t, r, :, 0:channels] = left.astype(bf16)
        buf_ref[c, t, r, :, channels : 2 * channels] = act.astype(bf16)
        buf_ref[c, t, r, :, 2 * channels : 3 * channels] = right.astype(bf16)

    for c in range(clips):
        at = [(j * clips + c) * 3 for j in (0, 1)]
        far_mean, far_square = [far[i : i + 1] + far[i + 1 : i + 2] + far[i + 2 : i + 3] for i in at]
        mean, inverse = merged(
            loc_ref[c : c + 1], loc_ref[clips + c : clips + c + 1], far_mean, far_square, members
        )
        scale = inverse * gain
        for t in range(frames):
            def row_step(r, carry):
                x = video_ref[c, t, r].astype(f32)
                put(c, t, r + 1, silu((x - mean) * scale))
                return carry

            lax.fori_loop(0, rows, row_step, 0, unroll=True)
            where_at = (c * frames + t) * cols
            halo = silu((pay_ref[where_at : where_at + cols].astype(f32) - mean) * scale)
            put(c, t, 0, jnp.where(strip > 0, halo, 0.0))
            put(c, t, rows + 1, jnp.where(strip > 0, 0.0, halo))

        def patches(t):
            return jnp.concatenate(
                [
                    buf_ref[c, t, b : b + rows].reshape(rows * cols, 3 * channels)
                    for b in range(3)
                ],
                axis=1,
            )

        for t in range(frames):
            total = video_ref[c, t].reshape(rows * cols, channels).astype(f32)
            for a in range(3):
                if t + a - 2 >= 0:
                    total = total + jnp.dot(
                        patches(t + a - 2), w_ref[a - first_tap], preferred_element_type=f32
                    )
            hid_ref[c, t * rows * cols : (t + 1) * rows * cols] = total

    def read(c, i):
        return hid_ref[c, i * cols : (i + 1) * cols]

    means, squares = local_stats(read, clips, frames * rows, cols, channels)
    st_ref[...] = stacked(
        [m[c : c + 1] for m in (means, squares) for c in range(clips)], channels
    )


def shard_bits():
    clip = lax.axis_index("clip")
    return ((clip & 1) << 2) | (((clip >> 1) & 1) << 1) | lax.axis_index("strip")


def tail_rows(count, extra=None):
    row = lax.broadcasted_iota(jnp.int32, (TAIL, 2 * LANES), 0)
    zero = jnp.zeros((1, LANES), f32)
    out = jnp.zeros((TAIL, 2 * LANES), f32)
    for i, value in enumerate((count,) if extra is None else (count, extra)):
        head, middle, last = [p.astype(f32) for p in pieces(value)]
        out = jnp.where(row == 2 * i, jnp.concatenate([head, middle], axis=1), out)
        out = jnp.where(row == 2 * i + 1, jnp.concatenate([last, zero], axis=1), out)
    return out.astype(bf16)


def untail(block, which=0):
    block = block.astype(f32)
    i = 2 * which
    return (
        block[i : i + 1, :LANES] + block[i : i + 1, LANES:] + block[i + 1 : i + 2, :LANES]
    )


def hot_rows(codes_ref, act_ref, acc_ref, first):
    share = LANES
    rows = acc_ref.shape[0]
    codes = codes_ref[...] ^ (shard_bits() * share)
    row_code = lax.broadcasted_iota(jnp.int32, (rows, LANES), 0) + first * share
    width = 2
    for k in range(codes.shape[0] // width):
        hot = []
        for j in range(width):
            line = codes[k * width + j : k * width + j + 1]
            hot.append(jnp.where(row_code == line, 1.0, 0.0).astype(bf16))
        part = jnp.dot(
            jnp.concatenate(hot, axis=1),
            act_ref[k * width * LANES : (k + 1) * width * LANES],
            preferred_element_type=f32,
        )
        if k == 0:
            acc_ref[...] = part
        else:
            acc_ref[...] += part


def hot_kernel(codes_ref, hot_ref):
    share = LANES
    rows = hot_ref.shape[0]
    codes = codes_ref[...] ^ (shard_bits() * share)
    row_code = lax.broadcasted_iota(jnp.int32, (rows, LANES), 0) + rows
    for k in range(codes.shape[0]):
        hot = jnp.where(row_code == codes[k : k + 1], 1.0, 0.0).astype(bf16)
        hot_ref[:, k * LANES : (k + 1) * LANES] = hot


def count_kernel(codes_ref, after_ref, cnt_ref, tails_ref, hot_ref):
    hot_kernel(codes_ref, hot_ref)
    share = LANES
    half = SHARDS // 2
    codes = codes_ref[...] ^ (shard_bits() * share)
    low_code = lax.broadcasted_iota(jnp.int32, (share, LANES), 0)
    high_code = lax.broadcasted_iota(jnp.int32, (SHARDS, LANES), 0)
    count = jnp.zeros((SHARDS, LANES), f32)
    shift = share.bit_length() - 1
    for k in range(codes.shape[0]):
        line = codes[k : k + 1]
        low = jnp.where(low_code == (line & (share - 1)), 1.0, 0.0).astype(bf16)
        high = jnp.where(high_code == (line >> shift), 1.0, 0.0).astype(bf16)
        count = count + lax.dot_general(
            high, low, (((1,), (1,)), ((), ())), preferred_element_type=f32
        )
    cnt_ref[...] = count
    for p in range(half):
        tails_ref[p] = tail_rows(count[half + p : half + p + 1])


def segment_kernel(
    hid_ref, near_ref, far_ref, gain_ref, hot_ref, tails_ref, act_ref, send_ref, acc_ref
):
    clips, tokens, channels = hid_ref.shape
    members = tokens * (channels // GROUPS)
    gain = gain_ref[...]
    block = 64
    for c in range(clips):
        mean, inverse = merged(
            near_ref[c : c + 1],
            near_ref[clips + c : clips + c + 1],
            far_ref[c : c + 1],
            far_ref[clips + c : clips + c + 1],
            members,
        )
        scale = inverse * gain
        for i in range(tokens // block):
            x = hid_ref[c, i * block : (i + 1) * block]
            act = silu((x - mean) * scale).astype(bf16)
            act_ref[c * tokens + i * block : c * tokens + (i + 1) * block] = act

    share = LANES
    half = SHARDS // 2
    width = act_ref.shape[0] // 2
    for k in range(2):
        at = slice(k * width, (k + 1) * width)
        part = jnp.dot(hot_ref[:, at], act_ref[at], preferred_element_type=f32)
        if k == 0:
            acc_ref[...] = part
        else:
            acc_ref[...] += part
    for p in range(half):
        send_ref[p, :share] = acc_ref[p * share : (p + 1) * share].astype(bf16)
        send_ref[p, share:] = tails_ref[p]


def keep_kernel(act_ref, codes_ref, keep_ref):
    hot_rows(codes_ref, act_ref, keep_ref, 0)


def quarter_kernel(keep_ref, cnt_ref, got_ref, mine_ref, mcnt_ref, s1_ref, s2_ref, s3_ref):
    share = LANES
    for p, out in enumerate((None, s1_ref, s2_ref, s3_ref)):
        value = keep_ref[p * share : (p + 1) * share] + got_ref[p, :share].astype(f32)
        count = cnt_ref[p : p + 1] + untail(got_ref[p, share:])
        if out is None:
            mine_ref[...] = value
            mcnt_ref[...] = jnp.broadcast_to(count, (8, LANES))
        else:
            out[:share] = value.astype(bf16)
            out[share:] = tail_rows(count)


def gathered_kernel(mine_ref, mcnt_ref, a_ref, b_ref, c_ref, after_ref, out_ref):
    share = mine_ref.shape[0]
    value = mine_ref[...]
    count = mcnt_ref[0:1]
    for ref in (a_ref, b_ref, c_ref):
        value = value + ref[:share].astype(f32)
        count = count + untail(ref[share:])
    out_ref[:share] = value.astype(bf16)
    out_ref[share:] = tail_rows(count)


def pair_kernel(own_ref, got_ref, out_ref):
    share = own_ref.shape[0] - TAIL
    value = own_ref[:share].astype(f32) + got_ref[:share].astype(f32)
    out_ref[:share] = value.astype(bf16)
    out_ref[share:] = tail_rows(untail(own_ref[share:]) + untail(got_ref[share:]))


def project_kernel(own_ref, got_ref, w_ref, err_ref, out_ref):
    share = own_ref.shape[0] - TAIL
    value = own_ref[:share].astype(f32) + got_ref[:share].astype(f32)
    head = value.astype(bf16)
    rest = (value - head.astype(f32)).astype(bf16)
    sums = jnp.dot(head, w_ref[...], preferred_element_type=f32) + jnp.dot(
        rest, w_ref[...], preferred_element_type=f32
    )
    out_ref[:share] = sums.astype(bf16)
    out_ref[share:] = tail_rows(
        untail(own_ref[share:]) + untail(got_ref[share:]), err_ref[0:1]
    )


def as_column(row):
    return jnp.transpose(jnp.broadcast_to(row, (LANES, LANES)))


def latent_kernel(act_ref, w_ref, codes_ref, sum_ref, cnt_ref, after_ref, lat_ref, err_ref, head_ref, rest_ref):
    tokens, channels = lat_ref.shape
    codes_count = sum_ref.shape[0]
    clips = 2
    counts = cnt_ref[...]
    grand = jnp.sum(counts)
    smooth = (counts + smooth_eps) / (grand + codes_count * smooth_eps) * grand
    for i in range(codes_count // LANES):
        divisor = as_column(smooth[i : i + 1])
        divisor = jnp.concatenate([divisor] * (channels // LANES), axis=1)
        book = sum_ref[i * LANES : (i + 1) * LANES] / divisor
        head = book.astype(bf16)
        head_ref[i * LANES : (i + 1) * LANES] = head
        rest_ref[i * LANES : (i + 1) * LANES] = (book - head.astype(f32)).astype(bf16)
    lane_code = lax.broadcasted_iota(jnp.int32, (LANES, codes_count), 1)
    lane = lax.broadcasted_iota(jnp.int32, (1, LANES), 1)
    lines = tokens // LANES
    per_clip = lines // clips
    errors = jnp.zeros((1, LANES), f32)
    for c in range(clips):
        def step(i, acc):
            line = c * per_clip + i
            at = pl.ds(pl.multiple_of(line * LANES, LANES), LANES)
            latent = jnp.dot(act_ref[at], w_ref[...], preferred_element_type=f32)
            lat_ref[at] = latent
            column = as_column(codes_ref[pl.ds(line, 1)])
            column = jnp.concatenate([column] * (codes_count // LANES), axis=1)
            hot = jnp.where(column == lane_code, 1.0, 0.0).astype(bf16)
            chosen = jnp.dot(hot, head_ref[...], preferred_element_type=f32) + jnp.dot(
                hot, rest_ref[...], preferred_element_type=f32
            )
            away = latent - chosen
            away = away * away
            return acc + jnp.sum(away.reshape(LANES // 8, 8, channels), axis=0)

        total = lax.fori_loop(0, per_clip, step, jnp.zeros((8, channels), f32), unroll=True)
        errors = jnp.where(lane == c, jnp.sum(total), errors)
    err_ref[...] = jnp.broadcast_to(errors, (8, LANES))


def book_kernel(first, tokens, *refs, done=lambda: None):
    parts, (sum_ref, cnt_ref), rest = refs[:-8], refs[-8:-6], refs[-6:]
    _, _, book_hbm, count_ref, page_ref, sems = rest
    me = shard_bits()
    share = LANES
    channels = sum_ref.shape[1]
    grand = ema_decay * jnp.sum(cnt_ref[...]) + (1.0 - ema_decay) * tokens
    copies = []
    for i in range(SHARDS // 2):
        src = parts[i] if len(parts) > 1 else parts[0].at[i]
        shard = (first + i) ^ me
        count = ema_decay * cnt_ref[pl.ds(shard, 1)] + (1.0 - ema_decay) * untail(src[share:])
        count_ref[i : i + 1] = count
        smooth = (count + smooth_eps) / (grand + SHARDS * share * smooth_eps) * grand
        inverse = as_column(1.0 / smooth)
        inverse = jnp.concatenate([inverse] * (channels // LANES), axis=1)
        at = pl.ds(pl.multiple_of(shard * share, share), share)
        fresh = ema_decay * sum_ref[at] + (1.0 - ema_decay) * src[:share].astype(f32)
        page_ref[i] = fresh * inverse
        copies.append(pltpu.make_async_copy(page_ref.at[i], book_hbm.at[at], sems.at[i]))
        copies[-1].start()
    done()
    for copy in copies:
        copy.wait()


def early_kernel(tokens, p0, p1, p2, p3, sum_ref, cnt_ref, book_hbm, count_ref, page_ref, sems):
    book_kernel(0, tokens, p0, p1, p2, p3, sum_ref, cnt_ref, None, None, book_hbm, count_ref, page_ref, sems)


def late_kernel(tokens, q_ref, sum_ref, cnt_ref, book_in, early_ref, book_hbm, count_hbm, page_ref, late_ref, line_ref, sems):
    half = SHARDS // 2
    copy = pltpu.make_async_copy(line_ref, count_hbm, sems.at[half])

    def counts():
        me = shard_bits()
        for i in range(half):
            line_ref[pl.ds(i ^ me, 1)] = early_ref[i : i + 1]
            line_ref[pl.ds((half + i) ^ me, 1)] = late_ref[i : i + 1]
        copy.start()

    book_kernel(
        half, tokens, q_ref, sum_ref, cnt_ref, None, None, book_hbm, late_ref, page_ref, sems, done=counts
    )
    copy.wait()


def error_kernel(scale, p1, err_ref, error_ref):
    error_ref[...] = jnp.broadcast_to(
        (err_ref[0:1] + untail(p1[LANES:], 1)) * scale, (8, LANES)
    )


def body(video, gain_first, conv_weight, gain_second, proj_weight, codes, ema_sum, ema_count):
    clips, frames, rows, cols, channels = video.shape
    codes_count = ema_sum.shape[0]
    clip_size, strips = lax.axis_size("clip"), lax.axis_size("strip")
    n = clip_size * strips
    share = codes_count // SHARDS
    assert strips == 2 and clip_size >= 4 and clip_size & (clip_size - 1) == 0
    assert share == LANES and channels == 2 * LANES and clips == 2

    def swap(x, mask):
        return lax.ppermute(x, BOTH, [(i, i ^ mask) for i in range(n)])

    tokens = frames * rows * cols
    halo = clips * frames * cols
    pay, near, held = call(
        stats_kernel,
        [
            ((halo + 16, channels), bf16),
            ((8, channels), f32),
            (video.shape, bf16),
        ],
        [pltpu.with_memory_space_constraint(video, pltpu.HBM)],
        scratch=[pltpu.SemaphoreType.DMA((clips,))],
        flops=10_000_000,
        limit=16 << 20,
        name="stats",
        far=(0,),
    )
    far_pay = swap(pay, 1)
    weights = pltpu.with_memory_space_constraint(
        conv_weight.reshape(3, 9 * channels, channels), pltpu.HBM
    )
    (taps,) = call(
        taps_kernel,
        [((min(3, frames), 9 * channels, channels), bf16)],
        [weights, near],
        scratch=[pltpu.SemaphoreType.DMA((1,))],
        flops=1_000_000_000,
        limit=8 << 20,
        name="taps",
        far=(0,),
    )
    hidden, near_two = call(
        conv_kernel,
        [((clips, tokens, channels), f32), ((8, channels), f32)],
        [held, far_pay, near, gain_first.reshape(1, channels), taps],
        scratch=[VMEM((clips, frames, rows + 2, cols, 3 * channels), bf16)],
        flops=4_000_000_000,
        limit=24 << 20,
        name="conv",
    )
    code_lines = lax.optimization_barrier((codes, near_two))[0].reshape(-1, LANES)
    far_two = swap(near_two, 1)
    cnt, tails, hot = call(
        count_kernel,
        [
            ((SHARDS, LANES), f32),
            ((SHARDS // 2, TAIL, channels), bf16),
            ((codes_count // 2, clips * tokens), bf16),
        ],
        [code_lines, near_two],
        flops=500_000_000,
        limit=8 << 20,
        name="count",
    )
    act, send = call(
        segment_kernel,
        [
            ((clips * tokens, channels), bf16),
            ((SHARDS // 2, share + TAIL, channels), bf16),
        ],
        [hidden, near_two, far_two, gain_second.reshape(1, channels), hot, tails],
        scratch=[VMEM((codes_count // 2, channels), f32)],
        flops=1_500_000_000,
        limit=24 << 20,
        name="segment",
    )
    core, x_bit = 2, 4
    got = swap(send, core)
    (keep,) = call(
        keep_kernel,
        [((codes_count // 2, channels), f32)],
        [act, code_lines],
        flops=1_000_000_000,
        limit=8 << 20,
        name="keep",
    )
    counts = ema_count.reshape(SHARDS, LANES)
    flat = ((share + TAIL, channels), bf16)
    mine, mine_cnt, s1, s2, s3 = call(
        quarter_kernel,
        [((share, channels), f32), ((8, LANES), f32), flat, flat, flat],
        [keep, cnt, got],
        flops=1_000_000,
        limit=8 << 20,
        name="quarter",
    )
    near_masks = (1, x_bit, 1 | x_bit)
    parts = [swap(s, m) for s, m in zip((s1, s2, s3), near_masks)]
    latent, err = call(
        latent_kernel,
        [((clips * tokens, channels), f32), ((8, LANES), f32)],
        [act, proj_weight, code_lines, ema_sum, counts, mine_cnt],
        scratch=[VMEM((codes_count, channels), bf16)] * 2,
        flops=2_500_000_000,
        limit=24 << 20,
        name="latent",
    )
    (own,) = call(
        gathered_kernel, [flat], [mine, mine_cnt, *parts, err], flops=1_000_000, limit=8 << 20, name="gathered"
    )
    bit = 8
    while bit < n // 2:
        (own,) = call(
            pair_kernel, [flat], [own, swap(own, bit)], flops=1_000_000, limit=8 << 20, name="pair"
        )
        bit *= 2
    last = swap(own, bit) if bit < n else jnp.zeros_like(own)
    (done,) = call(
        project_kernel, [flat], [own, last, proj_weight, err], flops=1_000_000, limit=8 << 20, name="project"
    )
    peers = [swap(done, m) for m in near_masks]
    across = swap(jnp.stack([done, *peers]), core)
    scale = 1.0 / (tokens * strips * channels)
    total_tokens = float(clips * tokens * n)
    half = SHARDS // 2
    (error,) = call(
        functools.partial(error_kernel, scale),
        [((8, LANES), f32)],
        [peers[0], err],
        flops=1_000_000,
        limit=8 << 20,
        name="error",
    )
    page = VMEM((half, share, channels), f32)
    book_shape = ((codes_count, channels), f32)
    book, early = call(
        functools.partial(early_kernel, total_tokens),
        [book_shape, ((8, LANES), f32)],
        [done, *peers, ema_sum, counts],
        scratch=[page, pltpu.SemaphoreType.DMA((half,))],
        flops=1_000_000,
        limit=8 << 20,
        name="early",
        far_outs=(0,),
    )
    book, count = call(
        functools.partial(late_kernel, total_tokens),
        [book_shape, ((SHARDS, LANES), f32)],
        [across, ema_sum, counts, book, early],
        scratch=[
            page,
            VMEM((8, LANES), f32),
            VMEM((SHARDS, LANES), f32),
            pltpu.SemaphoreType.DMA((half + 1,)),
        ],
        flops=1_000_000,
        limit=8 << 20,
        name="late",
        far=(3,),
        far_outs=(0, 1),
        alias={3: 0},
    )
    return (
        latent.reshape(clips, frames, rows, cols, channels),
        book,
        count.reshape(codes_count),
        error[0, :clips],
    )


def solution(mesh):
    in_specs = (
        P("clip", None, "strip", None, None),
        P(),
        P(),
        P(),
        P(),
        P("clip", None, "strip", None),
        P(),
        P(),
    )
    out_specs = (P("clip", None, "strip", None, None), P(), P(), P("clip"))
    return jax.shard_map(body, mesh=mesh, in_specs=in_specs, out_specs=out_specs, check_vma=False)
```

```python
import functools

import jax
import jax.numpy as jnp
from jax import lax
from jax.experimental import pallas as pl
from jax.experimental.pallas import tpu as pltpu
from jax.sharding import PartitionSpec as P

GROUPS = 32

norm_eps = 1e-06
smooth_eps = 1e-05
ema_decay = 0.9

f32 = jnp.float32
bf16 = jnp.bfloat16
LANES = 128
SHARDS = 8
TAIL = 8
BOTH = ("clip", "strip")
VMEM = pltpu.VMEM
VSPEC = pl.BlockSpec(memory_space=pltpu.VMEM)


def call(kernel, outs, args, scratch=(), flops=0, limit=None, name=None, far=(), far_outs=(), alias=None):
    far_spec = pl.BlockSpec(memory_space=pltpu.HBM)
    return pl.pallas_call(
        kernel,
        out_shape=tuple(jax.ShapeDtypeStruct(s, d) for s, d in outs),
        in_specs=[far_spec if i in far else VSPEC for i in range(len(args))],
        out_specs=tuple(far_spec if i in far_outs else VSPEC for i in range(len(outs))),
        scratch_shapes=list(scratch),
        input_output_aliases=alias or {},
        compiler_params=pltpu.CompilerParams(vmem_limit_bytes=limit),
        cost_estimate=pl.CostEstimate(flops=flops, bytes_accessed=0, transcendentals=0),
        name=name,
    )(*args)


def pieces(value):
    head = value.astype(bf16)
    rest = value - head.astype(f32)
    middle = rest.astype(bf16)
    last = (rest - middle.astype(f32)).astype(bf16)
    return head, middle, last


def group_matrix(channels):
    shift = (channels // GROUPS).bit_length() - 1
    rows = lax.broadcasted_iota(jnp.int32, (channels, channels), 0) >> shift
    cols = lax.broadcasted_iota(jnp.int32, (channels, channels), 1) >> shift
    return jnp.where(rows == cols, 1.0, 0.0).astype(bf16)


def group_total(rows, matrix):
    split = [p.astype(f32) for p in pieces(rows)]
    split = jnp.concatenate(split + [jnp.zeros_like(rows)], axis=0).astype(bf16)
    total = jnp.dot(split, matrix, preferred_element_type=f32)
    return total[0:8] + total[8:16] + total[16:24]


def stacked(rows, channels):
    row = lax.broadcasted_iota(jnp.int32, (8, channels), 0)
    out = jnp.zeros((8, channels), f32)
    for i, value in enumerate(rows):
        out = jnp.where(row == i, value, out)
    return out


def local_stats(read, clips, blocks, rows, channels, ready=lambda c: None):
    matrix = group_matrix(channels)
    members = blocks * rows * (channels // GROUPS)
    some = max(1, blocks // 8)

    def over(c, count, *terms):
        totals = []
        for term in terms:
            parts = [None] * 2
            for i in range(count):
                value = term(read(c, i))
                parts[i % 2] = value if parts[i % 2] is None else parts[i % 2] + value
            total = parts[0] if parts[1] is None else parts[0] + parts[1]
            totals.append(jnp.sum(total, axis=0, keepdims=True))
        return totals

    count = blocks * rows
    points, near, squares = [], [], []
    passes = []
    for c in range(clips):
        ready(c)
        point = over(c, some, lambda x: x)[0] * (1.0 / (some * rows))
        points.append(point)
        passes.append(over(c, blocks, lambda x: x - point, lambda x: (x - point) * (x - point)))
    pivot = group_total(stacked(points, channels), matrix) * (count / members)
    for c in range(clips):
        point = points[c]
        total, square = passes[c]
        apart = point - pivot[c : c + 1]
        near.append(total + count * apart)
        squares.append(square + 2.0 * apart * total + count * apart * apart)
    sums = near
    totals = group_total(stacked(sums + squares, channels), matrix)
    offset = totals[0:clips] / members
    square = jnp.maximum(totals[clips : 2 * clips] - totals[0:clips] * offset, 0.0)
    return pivot[0:clips] + offset, square


def merged(mean_a, square_a, mean_b, square_b, members):
    mean = 0.5 * (mean_a + mean_b)
    apart = mean_a - mean_b
    spread = (square_a + square_b + apart * apart * (0.5 * members)) / (2 * members)
    return mean, lax.rsqrt(spread + norm_eps)


def silu(v):
    half = 0.5 * v
    return half + half * jnp.tanh(half)


def taps_kernel(w_hbm, after_ref, w_ref, sem):
    first_tap = w_hbm.shape[0] - w_ref.shape[0]
    load = pltpu.make_async_copy(w_hbm.at[pl.ds(first_tap, w_ref.shape[0])], w_ref, sem.at[0])
    load.start()
    load.wait()


def stats_kernel(video_hbm, pay_ref, loc_ref, video_ref, sems):
    clips, frames, rows, cols, channels = video_ref.shape
    strip = lax.axis_index("strip")
    loads = [
        pltpu.make_async_copy(video_hbm.at[c], video_ref.at[c], sems.at[c]) for c in range(clips)
    ]
    for load in loads:
        load.start()

    def read(c, i):
        return video_ref[c, i // rows, i % rows].astype(f32)

    means, squares = local_stats(
        read, clips, frames * rows, cols, channels, ready=lambda c: loads[c].wait()
    )
    edge = (1 - strip) * (rows - 1)
    for c in range(clips):
        for t in range(frames):
            at = (c * frames + t) * cols
            pay_ref[at : at + cols] = video_ref[c, t, edge]

    loc_ref[...] = stacked([m[c : c + 1] for m in (means, squares) for c in range(clips)], channels)
    base = clips * frames * cols
    row = lax.broadcasted_iota(jnp.int32, (16, channels), 0)
    out = jnp.zeros((16, channels), f32)
    for j, value in enumerate((means, squares)):
        for k, piece in enumerate(pieces(value)):
            piece = piece.astype(f32)
            for c in range(clips):
                out = jnp.where(row == (j * clips + c) * 3 + k, piece[c : c + 1], out)
    pay_ref[base : base + 16] = out.astype(bf16)


def conv_kernel(video_ref, pay_ref, loc_ref, gain_ref, w_ref, hid_ref, st_ref, buf_ref):
    clips, frames, rows, cols, channels = video_ref.shape
    strip = lax.axis_index("strip")
    members = frames * rows * cols * (channels // GROUPS)
    base = clips * frames * cols
    first_tap = 3 - w_ref.shape[0]
    far = pay_ref[base : base + 16].astype(f32)
    gain = gain_ref[...]
    col = lax.broadcasted_iota(jnp.int32, (cols, channels), 0)

    def put(c, t, r, act):
        left = jnp.where(col == 0, 0.0, pltpu.roll(act, 1, 0))
        right = jnp.where(col == cols - 1, 0.0, pltpu.roll(act, cols - 1, 0))
        buf_ref[c, t, r, :, 0:channels] = left.astype(bf16)
        buf_ref[c, t, r, :, channels : 2 * channels] = act.astype(bf16)
        buf_ref[c, t, r, :, 2 * channels : 3 * channels] = right.astype(bf16)

    for c in range(clips):
        at = [(j * clips + c) * 3 for j in (0, 1)]
        far_mean, far_square = [far[i : i + 1] + far[i + 1 : i + 2] + far[i + 2 : i + 3] for i in at]
        mean, inverse = merged(
            loc_ref[c : c + 1], loc_ref[clips + c : clips + c + 1], far_mean, far_square, members
        )
        scale = inverse * gain
        for t in range(frames):
            def row_step(r, carry):
                x = video_ref[c, t, r].astype(f32)
                put(c, t, r + 1, silu((x - mean) * scale))
                return carry

            lax.fori_loop(0, rows, row_step, 0, unroll=True)
            where_at = (c * frames + t) * cols
            halo = silu((pay_ref[where_at : where_at + cols].astype(f32) - mean) * scale)
            put(c, t, 0, jnp.where(strip > 0, halo, 0.0))
            put(c, t, rows + 1, jnp.where(strip > 0, 0.0, halo))

        def patches(t):
            return jnp.concatenate(
                [
                    buf_ref[c, t, b : b + rows].reshape(rows * cols, 3 * channels)
                    for b in range(3)
                ],
                axis=1,
            )

        for t in range(frames):
            total = video_ref[c, t].reshape(rows * cols, channels).astype(f32)
            for a in range(3):
                if t + a - 2 >= 0:
                    total = total + jnp.dot(
                        patches(t + a - 2), w_ref[a - first_tap], preferred_element_type=f32
                    )
            hid_ref[c, t * rows * cols : (t + 1) * rows * cols] = total

    def read(c, i):
        return hid_ref[c, i * cols : (i + 1) * cols]

    means, squares = local_stats(read, clips, frames * rows, cols, channels)
    st_ref[...] = stacked(
        [m[c : c + 1] for m in (means, squares) for c in range(clips)], channels
    )


def shard_bits():
    clip = lax.axis_index("clip")
    return ((clip & 1) << 2) | (((clip >> 1) & 1) << 1) | lax.axis_index("strip")


def tail_rows(count, extra=None):
    row = lax.broadcasted_iota(jnp.int32, (TAIL, 2 * LANES), 0)
    zero = jnp.zeros((1, LANES), f32)
    out = jnp.zeros((TAIL, 2 * LANES), f32)
    for i, value in enumerate((count,) if extra is None else (count, extra)):
        head, middle, last = [p.astype(f32) for p in pieces(value)]
        out = jnp.where(row == 2 * i, jnp.concatenate([head, middle], axis=1), out)
        out = jnp.where(row == 2 * i + 1, jnp.concatenate([last, zero], axis=1), out)
    return out.astype(bf16)


def untail(block, which=0):
    block = block.astype(f32)
    i = 2 * which
    return (
        block[i : i + 1, :LANES] + block[i : i + 1, LANES:] + block[i + 1 : i + 2, :LANES]
    )


def hot_rows(codes_ref, act_ref, acc_ref, first):
    share = LANES
    rows = acc_ref.shape[0]
    codes = codes_ref[...] ^ (shard_bits() * share)
    row_code = lax.broadcasted_iota(jnp.int32, (rows, LANES), 0) + first * share
    width = 2
    for k in range(codes.shape[0] // width):
        hot = []
        for j in range(width):
            line = codes[k * width + j : k * width + j + 1]
            hot.append(jnp.where(row_code == line, 1.0, 0.0).astype(bf16))
        part = jnp.dot(
            jnp.concatenate(hot, axis=1),
            act_ref[k * width * LANES : (k + 1) * width * LANES],
            preferred_element_type=f32,
        )
        if k == 0:
            acc_ref[...] = part
        else:
            acc_ref[...] += part


def hot_kernel(codes_ref, hot_ref):
    share = LANES
    rows = hot_ref.shape[0]
    codes = codes_ref[...] ^ (shard_bits() * share)
    row_code = lax.broadcasted_iota(jnp.int32, (rows, LANES), 0) + rows
    for k in range(codes.shape[0]):
        hot = jnp.where(row_code == codes[k : k + 1], 1.0, 0.0).astype(bf16)
        hot_ref[:, k * LANES : (k + 1) * LANES] = hot


def count_kernel(codes_ref, after_ref, cnt_ref, tails_ref, hot_ref):
    hot_kernel(codes_ref, hot_ref)
    share = LANES
    half = SHARDS // 2
    codes = codes_ref[...] ^ (shard_bits() * share)
    low_code = lax.broadcasted_iota(jnp.int32, (share, LANES), 0)
    high_code = lax.broadcasted_iota(jnp.int32, (SHARDS, LANES), 0)
    count = jnp.zeros((SHARDS, LANES), f32)
    shift = share.bit_length() - 1
    for k in range(codes.shape[0]):
        line = codes[k : k + 1]
        low = jnp.where(low_code == (line & (share - 1)), 1.0, 0.0).astype(bf16)
        high = jnp.where(high_code == (line >> shift), 1.0, 0.0).astype(bf16)
        count = count + lax.dot_general(
            high, low, (((1,), (1,)), ((), ())), preferred_element_type=f32
        )
    cnt_ref[...] = count
    for p in range(half):
        tails_ref[p] = tail_rows(count[half + p : half + p + 1])


def segment_kernel(
    hid_ref, near_ref, far_ref, gain_ref, hot_ref, tails_ref, act_ref, send_ref, acc_ref
):
    clips, tokens, channels = hid_ref.shape
    members = tokens * (channels // GROUPS)
    gain = gain_ref[...]
    block = 64
    for c in range(clips):
        mean, inverse = merged(
            near_ref[c : c + 1],
            near_ref[clips + c : clips + c + 1],
            far_ref[c : c + 1],
            far_ref[clips + c : clips + c + 1],
            members,
        )
        scale = inverse * gain
        for i in range(tokens // block):
            x = hid_ref[c, i * block : (i + 1) * block]
            act = silu((x - mean) * scale).astype(bf16)
            act_ref[c * tokens + i * block : c * tokens + (i + 1) * block] = act

    share = LANES
    half = SHARDS // 2
    width = act_ref.shape[0] // 2
    for k in range(2):
        at = slice(k * width, (k + 1) * width)
        part = jnp.dot(hot_ref[:, at], act_ref[at], preferred_element_type=f32)
        if k == 0:
            acc_ref[...] = part
        else:
            acc_ref[...] += part
    for p in range(half):
        send_ref[p, :share] = acc_ref[p * share : (p + 1) * share].astype(bf16)
        send_ref[p, share:] = tails_ref[p]


def keep_kernel(act_ref, codes_ref, keep_ref):
    hot_rows(codes_ref, act_ref, keep_ref, 0)


def quarter_kernel(keep_ref, cnt_ref, got_ref, mine_ref, mcnt_ref, s1_ref, s2_ref, s3_ref):
    share = LANES
    for p, out in enumerate((None, s1_ref, s2_ref, s3_ref)):
        value = keep_ref[p * share : (p + 1) * share] + got_ref[p, :share].astype(f32)
        count = cnt_ref[p : p + 1] + untail(got_ref[p, share:])
        if out is None:
            mine_ref[...] = value
            mcnt_ref[...] = jnp.broadcast_to(count, (8, LANES))
        else:
            out[:share] = value.astype(bf16)
            out[share:] = tail_rows(count)


def gathered_kernel(mine_ref, mcnt_ref, a_ref, b_ref, c_ref, after_ref, out_ref):
    share = mine_ref.shape[0]
    value = mine_ref[...]
    count = mcnt_ref[0:1]
    for ref in (a_ref, b_ref, c_ref):
        value = value + ref[:share].astype(f32)
        count = count + untail(ref[share:])
    out_ref[:share] = value.astype(bf16)
    out_ref[share:] = tail_rows(count)


def pair_kernel(own_ref, got_ref, out_ref):
    share = own_ref.shape[0] - TAIL
    value = own_ref[:share].astype(f32) + got_ref[:share].astype(f32)
    out_ref[:share] = value.astype(bf16)
    out_ref[share:] = tail_rows(untail(own_ref[share:]) + untail(got_ref[share:]))


def project_kernel(own_ref, got_ref, w_ref, err_ref, out_ref):
    share = own_ref.shape[0] - TAIL
    value = own_ref[:share].astype(f32) + got_ref[:share].astype(f32)
    head = value.astype(bf16)
    rest = (value - head.astype(f32)).astype(bf16)
    sums = jnp.dot(head, w_ref[...], preferred_element_type=f32) + jnp.dot(
        rest, w_ref[...], preferred_element_type=f32
    )
    out_ref[:share] = sums.astype(bf16)
    out_ref[share:] = tail_rows(
        untail(own_ref[share:]) + untail(got_ref[share:]), err_ref[0:1]
    )


def as_column(row):
    return jnp.transpose(jnp.broadcast_to(row, (LANES, LANES)))


def latent_kernel(act_ref, w_ref, codes_ref, sum_ref, cnt_ref, after_ref, lat_ref, err_ref, head_ref, rest_ref):
    tokens, channels = lat_ref.shape
    codes_count = sum_ref.shape[0]
    clips = 2
    counts = cnt_ref[...]
    grand = jnp.sum(counts)
    smooth = (counts + smooth_eps) / (grand + codes_count * smooth_eps) * grand
    for i in range(codes_count // LANES):
        divisor = as_column(smooth[i : i + 1])
        divisor = jnp.concatenate([divisor] * (channels // LANES), axis=1)
        book = sum_ref[i * LANES : (i + 1) * LANES] / divisor
        head = book.astype(bf16)
        head_ref[i * LANES : (i + 1) * LANES] = head
        rest_ref[i * LANES : (i + 1) * LANES] = (book - head.astype(f32)).astype(bf16)
    lane_code = lax.broadcasted_iota(jnp.int32, (LANES, codes_count), 1)
    lane = lax.broadcasted_iota(jnp.int32, (1, LANES), 1)
    lines = tokens // LANES
    per_clip = lines // clips
    errors = jnp.zeros((1, LANES), f32)
    for c in range(clips):
        def step(i, acc):
            line = c * per_clip + i
            at = pl.ds(pl.multiple_of(line * LANES, LANES), LANES)
            latent = jnp.dot(act_ref[at], w_ref[...], preferred_element_type=f32)
            lat_ref[at] = latent
            column = as_column(codes_ref[pl.ds(line, 1)])
            column = jnp.concatenate([column] * (codes_count // LANES), axis=1)
            hot = jnp.where(column == lane_code, 1.0, 0.0).astype(bf16)
            chosen = jnp.dot(hot, head_ref[...], preferred_element_type=f32) + jnp.dot(
                hot, rest_ref[...], preferred_element_type=f32
            )
            away = latent - chosen
            away = away * away
            return acc + jnp.sum(away.reshape(LANES // 8, 8, channels), axis=0)

        total = lax.fori_loop(0, per_clip, step, jnp.zeros((8, channels), f32), unroll=True)
        errors = jnp.where(lane == c, jnp.sum(total), errors)
    err_ref[...] = jnp.broadcast_to(errors, (8, LANES))


def book_kernel(first, tokens, *refs, done=lambda: None):
    parts, (sum_ref, cnt_ref), rest = refs[:-8], refs[-8:-6], refs[-6:]
    _, _, book_hbm, count_ref, page_ref, sems = rest
    me = shard_bits()
    share = LANES
    channels = sum_ref.shape[1]
    grand = ema_decay * jnp.sum(cnt_ref[...]) + (1.0 - ema_decay) * tokens
    copies = []
    for i in range(SHARDS // 2):
        src = parts[i] if len(parts) > 1 else parts[0].at[i]
        shard = (first + i) ^ me
        count = ema_decay * cnt_ref[pl.ds(shard, 1)] + (1.0 - ema_decay) * untail(src[share:])
        count_ref[i : i + 1] = count
        smooth = (count + smooth_eps) / (grand + SHARDS * share * smooth_eps) * grand
        inverse = as_column(1.0 / smooth)
        inverse = jnp.concatenate([inverse] * (channels // LANES), axis=1)
        at = pl.ds(pl.multiple_of(shard * share, share), share)
        fresh = ema_decay * sum_ref[at] + (1.0 - ema_decay) * src[:share].astype(f32)
        page_ref[i] = fresh * inverse
        copies.append(pltpu.make_async_copy(page_ref.at[i], book_hbm.at[at], sems.at[i]))
        copies[-1].start()
    done()
    for copy in copies:
        copy.wait()


def early_kernel(
    tokens, scale, p0, p1, p2, p3, sum_ref, cnt_ref, err_ref, book_hbm, count_ref, error_hbm, page_ref, error_ref, sems
):
    copy = pltpu.make_async_copy(error_ref, error_hbm, sems.at[SHARDS // 2])
    errors = (err_ref[0:1] + untail(p1[LANES:], 1)) * scale
    error_ref[...] = errors[0, : error_ref.shape[0]]
    copy.start()
    book_kernel(0, tokens, p0, p1, p2, p3, sum_ref, cnt_ref, None, None, book_hbm, count_ref, page_ref, sems)
    copy.wait()


def late_kernel(
    tokens, q0, q1, q2, q3, sum_ref, cnt_ref, book_in, early_ref, book_hbm, count_hbm, page_ref, late_ref, line_ref, sems
):
    half = SHARDS // 2
    copy = pltpu.make_async_copy(line_ref, count_hbm, sems.at[half])

    def counts():
        me = shard_bits()
        for i in range(half):
            line_ref[pl.ds(i ^ me, 1)] = early_ref[i : i + 1]
            line_ref[pl.ds((half + i) ^ me, 1)] = late_ref[i : i + 1]
        copy.start()

    book_kernel(
        half, tokens, q0, q1, q2, q3, sum_ref, cnt_ref, None, None, book_hbm, late_ref, page_ref, sems, done=counts
    )
    copy.wait()


def body(video, gain_first, conv_weight, gain_second, proj_weight, codes, ema_sum, ema_count):
    clips, frames, rows, cols, channels = video.shape
    codes_count = ema_sum.shape[0]
    clip_size, strips = lax.axis_size("clip"), lax.axis_size("strip")
    n = clip_size * strips
    share = codes_count // SHARDS
    assert strips == 2 and clip_size >= 4 and clip_size & (clip_size - 1) == 0
    assert share == LANES and channels == 2 * LANES and clips == 2

    def swap(x, mask):
        return lax.ppermute(x, BOTH, [(i, i ^ mask) for i in range(n)])

    tokens = frames * rows * cols
    halo = clips * frames * cols
    pay, near, held = call(
        stats_kernel,
        [
            ((halo + 16, channels), bf16),
            ((8, channels), f32),
            (video.shape, bf16),
        ],
        [pltpu.with_memory_space_constraint(video, pltpu.HBM)],
        scratch=[pltpu.SemaphoreType.DMA((clips,))],
        flops=10_000_000,
        limit=16 << 20,
        name="stats",
        far=(0,),
    )
    far_pay = swap(pay, 1)
    weights = pltpu.with_memory_space_constraint(
        conv_weight.reshape(3, 9 * channels, channels), pltpu.HBM
    )
    (taps,) = call(
        taps_kernel,
        [((min(3, frames), 9 * channels, channels), bf16)],
        [weights, near],
        scratch=[pltpu.SemaphoreType.DMA((1,))],
        flops=1_000_000_000,
        limit=8 << 20,
        name="taps",
        far=(0,),
    )
    hidden, near_two = call(
        conv_kernel,
        [((clips, tokens, channels), f32), ((8, channels), f32)],
        [held, far_pay, near, gain_first.reshape(1, channels), taps],
        scratch=[VMEM((clips, frames, rows + 2, cols, 3 * channels), bf16)],
        flops=4_000_000_000,
        limit=24 << 20,
        name="conv",
    )
    code_lines = lax.optimization_barrier((codes, near_two))[0].reshape(-1, LANES)
    far_two = swap(near_two, 1)
    cnt, tails, hot = call(
        count_kernel,
        [
            ((SHARDS, LANES), f32),
            ((SHARDS // 2, TAIL, channels), bf16),
            ((codes_count // 2, clips * tokens), bf16),
        ],
        [code_lines, near_two],
        flops=500_000_000,
        limit=8 << 20,
        name="count",
    )
    act, send = call(
        segment_kernel,
        [
            ((clips * tokens, channels), bf16),
            ((SHARDS // 2, share + TAIL, channels), bf16),
        ],
        [hidden, near_two, far_two, gain_second.reshape(1, channels), hot, tails],
        scratch=[VMEM((codes_count // 2, channels), f32)],
        flops=1_500_000_000,
        limit=24 << 20,
        name="segment",
    )
    core, x_bit = 2, 4
    got = swap(send, core)
    (keep,) = call(
        keep_kernel,
        [((codes_count // 2, channels), f32)],
        [act, code_lines],
        flops=1_000_000_000,
        limit=8 << 20,
        name="keep",
    )
    counts = ema_count.reshape(SHARDS, LANES)
    flat = ((share + TAIL, channels), bf16)
    mine, mine_cnt, s1, s2, s3 = call(
        quarter_kernel,
        [((share, channels), f32), ((8, LANES), f32), flat, flat, flat],
        [keep, cnt, got],
        flops=1_000_000,
        limit=8 << 20,
        name="quarter",
    )
    near_masks = (1, x_bit, 1 | x_bit)
    parts = [swap(s, m) for s, m in zip((s1, s2, s3), near_masks)]
    latent, err = call(
        latent_kernel,
        [((clips * tokens, channels), f32), ((8, LANES), f32)],
        [act, proj_weight, code_lines, ema_sum, counts, mine_cnt],
        scratch=[VMEM((codes_count, channels), bf16)] * 2,
        flops=2_500_000_000,
        limit=24 << 20,
        name="latent",
    )
    (own,) = call(
        gathered_kernel, [flat], [mine, mine_cnt, *parts, err], flops=1_000_000, limit=8 << 20, name="gathered"
    )
    bit = 8
    while bit < n // 2:
        (own,) = call(
            pair_kernel, [flat], [own, swap(own, bit)], flops=1_000_000, limit=8 << 20, name="pair"
        )
        bit *= 2
    last = swap(own, bit) if bit < n else jnp.zeros_like(own)
    (done,) = call(
        project_kernel, [flat], [own, last, proj_weight, err], flops=1_000_000, limit=8 << 20, name="project"
    )
    peers = [swap(done, m) for m in near_masks]
    across = [swap(part, core) for part in (done, *peers)]
    scale = 1.0 / (tokens * strips * channels)
    total_tokens = float(clips * tokens * n)
    half = SHARDS // 2
    page = VMEM((half, share, channels), f32)
    book_shape = ((codes_count, channels), f32)
    book, early, error = call(
        functools.partial(early_kernel, total_tokens, scale),
        [book_shape, ((8, LANES), f32), ((clips,), f32)],
        [done, *peers, ema_sum, counts, err],
        scratch=[page, VMEM((clips,), f32), pltpu.SemaphoreType.DMA((half + 1,))],
        flops=1_000_000,
        limit=8 << 20,
        name="early",
        far_outs=(0, 2),
    )
    book, count = call(
        functools.partial(late_kernel, total_tokens),
        [book_shape, ((SHARDS, LANES), f32)],
        [*across, ema_sum, counts, book, early],
        scratch=[
            page,
            VMEM((8, LANES), f32),
            VMEM((SHARDS, LANES), f32),
            pltpu.SemaphoreType.DMA((half + 1,)),
        ],
        flops=1_000_000,
        limit=8 << 20,
        name="late",
        far=(half + 2,),
        far_outs=(0, 1),
        alias={half + 2: 0},
    )
    return (
        latent.reshape(clips, frames, rows, cols, channels),
        book,
        count.reshape(codes_count),
        error,
    )


def solution(mesh):
    in_specs = (
        P("clip", None, "strip", None, None),
        P(),
        P(),
        P(),
        P(),
        P("clip", None, "strip", None),
        P(),
        P(),
    )
    out_specs = (P("clip", None, "strip", None, None), P(), P(), P("clip"))
    return jax.shard_map(body, mesh=mesh, in_specs=in_specs, out_specs=out_specs, check_vma=False)
```

```python
import functools

import jax
import jax.numpy as jnp
from jax import lax
from jax.experimental import pallas as pl
from jax.experimental.pallas import tpu as pltpu
from jax.sharding import PartitionSpec as P

GROUPS = 32

norm_eps = 1e-06
smooth_eps = 1e-05
ema_decay = 0.9

f32 = jnp.float32
bf16 = jnp.bfloat16
LANES = 128
SHARDS = 8
TAIL = 8
BOTH = ("clip", "strip")
VMEM = pltpu.VMEM
VSPEC = pl.BlockSpec(memory_space=pltpu.VMEM)


def call(kernel, outs, args, scratch=(), flops=0, limit=None, name=None, far=(), far_outs=(), alias=None):
    far_spec = pl.BlockSpec(memory_space=pltpu.HBM)
    return pl.pallas_call(
        kernel,
        out_shape=tuple(jax.ShapeDtypeStruct(s, d) for s, d in outs),
        in_specs=[far_spec if i in far else VSPEC for i in range(len(args))],
        out_specs=tuple(far_spec if i in far_outs else VSPEC for i in range(len(outs))),
        scratch_shapes=list(scratch),
        input_output_aliases=alias or {},
        compiler_params=pltpu.CompilerParams(vmem_limit_bytes=limit),
        cost_estimate=pl.CostEstimate(flops=flops, bytes_accessed=0, transcendentals=0),
        name=name,
    )(*args)


def pieces(value):
    head = value.astype(bf16)
    rest = value - head.astype(f32)
    middle = rest.astype(bf16)
    last = (rest - middle.astype(f32)).astype(bf16)
    return head, middle, last


def group_matrix(channels):
    shift = (channels // GROUPS).bit_length() - 1
    rows = lax.broadcasted_iota(jnp.int32, (channels, channels), 0) >> shift
    cols = lax.broadcasted_iota(jnp.int32, (channels, channels), 1) >> shift
    return jnp.where(rows == cols, 1.0, 0.0).astype(bf16)


def group_total(rows, matrix):
    split = [p.astype(f32) for p in pieces(rows)]
    split = jnp.concatenate(split + [jnp.zeros_like(rows)], axis=0).astype(bf16)
    total = jnp.dot(split, matrix, preferred_element_type=f32)
    return total[0:8] + total[8:16] + total[16:24]


def stacked(rows, channels):
    row = lax.broadcasted_iota(jnp.int32, (8, channels), 0)
    out = jnp.zeros((8, channels), f32)
    for i, value in enumerate(rows):
        out = jnp.where(row == i, value, out)
    return out


def local_stats(read, clips, blocks, rows, channels, ready=lambda c: None):
    matrix = group_matrix(channels)
    members = blocks * rows * (channels // GROUPS)
    some = max(1, blocks // 8)

    def over(c, count, *terms):
        totals = []
        for term in terms:
            parts = [None] * 2
            for i in range(count):
                value = term(read(c, i))
                parts[i % 2] = value if parts[i % 2] is None else parts[i % 2] + value
            total = parts[0] if parts[1] is None else parts[0] + parts[1]
            totals.append(jnp.sum(total, axis=0, keepdims=True))
        return totals

    count = blocks * rows
    points, near, squares = [], [], []
    passes = []
    for c in range(clips):
        ready(c)
        point = over(c, some, lambda x: x)[0] * (1.0 / (some * rows))
        points.append(point)
        passes.append(over(c, blocks, lambda x: x - point, lambda x: (x - point) * (x - point)))
    pivot = group_total(stacked(points, channels), matrix) * (count / members)
    for c in range(clips):
        point = points[c]
        total, square = passes[c]
        apart = point - pivot[c : c + 1]
        near.append(total + count * apart)
        squares.append(square + 2.0 * apart * total + count * apart * apart)
    sums = near
    totals = group_total(stacked(sums + squares, channels), matrix)
    offset = totals[0:clips] / members
    square = jnp.maximum(totals[clips : 2 * clips] - totals[0:clips] * offset, 0.0)
    return pivot[0:clips] + offset, square


def merged(mean_a, square_a, mean_b, square_b, members):
    mean = 0.5 * (mean_a + mean_b)
    apart = mean_a - mean_b
    spread = (square_a + square_b + apart * apart * (0.5 * members)) / (2 * members)
    return mean, lax.rsqrt(spread + norm_eps)


def silu(v):
    half = 0.5 * v
    return half + half * jnp.tanh(half)


def taps_kernel(w_hbm, after_ref, w_ref, sem):
    first_tap = w_hbm.shape[0] - w_ref.shape[0]
    load = pltpu.make_async_copy(w_hbm.at[pl.ds(first_tap, w_ref.shape[0])], w_ref, sem.at[0])
    load.start()
    load.wait()


def stats_kernel(video_hbm, pay_ref, loc_ref, video_ref, sems):
    clips, frames, rows, cols, channels = video_ref.shape
    strip = lax.axis_index("strip")
    loads = [
        pltpu.make_async_copy(video_hbm.at[c], video_ref.at[c], sems.at[c]) for c in range(clips)
    ]
    for load in loads:
        load.start()

    def read(c, i):
        return video_ref[c, i // rows, i % rows].astype(f32)

    means, squares = local_stats(
        read, clips, frames * rows, cols, channels, ready=lambda c: loads[c].wait()
    )
    edge = (1 - strip) * (rows - 1)
    for c in range(clips):
        for t in range(frames):
            at = (c * frames + t) * cols
            pay_ref[at : at + cols] = video_ref[c, t, edge]

    loc_ref[...] = stacked([m[c : c + 1] for m in (means, squares) for c in range(clips)], channels)
    base = clips * frames * cols
    row = lax.broadcasted_iota(jnp.int32, (16, channels), 0)
    out = jnp.zeros((16, channels), f32)
    for j, value in enumerate((means, squares)):
        for k, piece in enumerate(pieces(value)):
            piece = piece.astype(f32)
            for c in range(clips):
                out = jnp.where(row == (j * clips + c) * 3 + k, piece[c : c + 1], out)
    pay_ref[base : base + 16] = out.astype(bf16)


def conv_kernel(video_ref, pay_ref, loc_ref, gain_ref, w_ref, hid_ref, st_ref, buf_ref):
    clips, frames, rows, cols, channels = video_ref.shape
    strip = lax.axis_index("strip")
    members = frames * rows * cols * (channels // GROUPS)
    base = clips * frames * cols
    first_tap = 3 - w_ref.shape[0]
    far = pay_ref[base : base + 16].astype(f32)
    gain = gain_ref[...]
    col = lax.broadcasted_iota(jnp.int32, (cols, channels), 0)

    def put(c, t, r, act):
        left = jnp.where(col == 0, 0.0, pltpu.roll(act, 1, 0))
        right = jnp.where(col == cols - 1, 0.0, pltpu.roll(act, cols - 1, 0))
        buf_ref[c, t, r, :, 0:channels] = left.astype(bf16)
        buf_ref[c, t, r, :, channels : 2 * channels] = act.astype(bf16)
        buf_ref[c, t, r, :, 2 * channels : 3 * channels] = right.astype(bf16)

    for c in range(clips):
        at = [(j * clips + c) * 3 for j in (0, 1)]
        far_mean, far_square = [far[i : i + 1] + far[i + 1 : i + 2] + far[i + 2 : i + 3] for i in at]
        mean, inverse = merged(
            loc_ref[c : c + 1], loc_ref[clips + c : clips + c + 1], far_mean, far_square, members
        )
        scale = inverse * gain
        for t in range(frames):
            def row_step(r, carry):
                x = video_ref[c, t, r].astype(f32)
                put(c, t, r + 1, silu((x - mean) * scale))
                return carry

            lax.fori_loop(0, rows, row_step, 0, unroll=True)
            where_at = (c * frames + t) * cols
            halo = silu((pay_ref[where_at : where_at + cols].astype(f32) - mean) * scale)
            put(c, t, 0, jnp.where(strip > 0, halo, 0.0))
            put(c, t, rows + 1, jnp.where(strip > 0, 0.0, halo))

        def patches(t):
            return [
                buf_ref[c, t, b : b + rows].reshape(rows * cols, 3 * channels) for b in range(3)
            ]

        for t in range(frames):
            total = video_ref[c, t].reshape(rows * cols, channels).astype(f32)
            for a in range(3):
                if t + a - 2 >= 0:
                    for b, part in enumerate(patches(t + a - 2)):
                        rows_at = slice(b * 3 * channels, (b + 1) * 3 * channels)
                        total = total + jnp.dot(
                            part, w_ref[a - first_tap, rows_at], preferred_element_type=f32
                        )
            hid_ref[c, t * rows * cols : (t + 1) * rows * cols] = total

    def read(c, i):
        return hid_ref[c, i * cols : (i + 1) * cols]

    means, squares = local_stats(read, clips, frames * rows, cols, channels)
    st_ref[...] = stacked(
        [m[c : c + 1] for m in (means, squares) for c in range(clips)], channels
    )


def shard_bits():
    clip = lax.axis_index("clip")
    return ((clip & 1) << 2) | (((clip >> 1) & 1) << 1) | lax.axis_index("strip")


def tail_rows(count, extra=None):
    row = lax.broadcasted_iota(jnp.int32, (TAIL, 2 * LANES), 0)
    zero = jnp.zeros((1, LANES), f32)
    out = jnp.zeros((TAIL, 2 * LANES), f32)
    for i, value in enumerate((count,) if extra is None else (count, extra)):
        head, middle, last = [p.astype(f32) for p in pieces(value)]
        out = jnp.where(row == 2 * i, jnp.concatenate([head, middle], axis=1), out)
        out = jnp.where(row == 2 * i + 1, jnp.concatenate([last, zero], axis=1), out)
    return out.astype(bf16)


def untail(block, which=0):
    block = block.astype(f32)
    i = 2 * which
    return (
        block[i : i + 1, :LANES] + block[i : i + 1, LANES:] + block[i + 1 : i + 2, :LANES]
    )


def hot_rows(codes_ref, act_ref, acc_ref, first):
    share = LANES
    rows = acc_ref.shape[0]
    codes = codes_ref[...] ^ (shard_bits() * share)
    row_code = lax.broadcasted_iota(jnp.int32, (rows, LANES), 0) + first * share
    width = 2
    for k in range(codes.shape[0] // width):
        hot = []
        for j in range(width):
            line = codes[k * width + j : k * width + j + 1]
            hot.append(jnp.where(row_code == line, 1.0, 0.0).astype(bf16))
        part = jnp.dot(
            jnp.concatenate(hot, axis=1),
            act_ref[k * width * LANES : (k + 1) * width * LANES],
            preferred_element_type=f32,
        )
        if k == 0:
            acc_ref[...] = part
        else:
            acc_ref[...] += part


def hot_kernel(codes_ref, hot_ref):
    share = LANES
    rows = hot_ref.shape[0]
    codes = codes_ref[...] ^ (shard_bits() * share)
    row_code = lax.broadcasted_iota(jnp.int32, (rows, LANES), 0) + rows
    for k in range(codes.shape[0]):
        hot = jnp.where(row_code == codes[k : k + 1], 1.0, 0.0).astype(bf16)
        hot_ref[:, k * LANES : (k + 1) * LANES] = hot


def count_kernel(codes_ref, after_ref, cnt_ref, tails_ref, hot_ref):
    hot_kernel(codes_ref, hot_ref)
    share = LANES
    half = SHARDS // 2
    codes = codes_ref[...] ^ (shard_bits() * share)
    low_code = lax.broadcasted_iota(jnp.int32, (share, LANES), 0)
    high_code = lax.broadcasted_iota(jnp.int32, (SHARDS, LANES), 0)
    count = jnp.zeros((SHARDS, LANES), f32)
    shift = share.bit_length() - 1
    for k in range(codes.shape[0]):
        line = codes[k : k + 1]
        low = jnp.where(low_code == (line & (share - 1)), 1.0, 0.0).astype(bf16)
        high = jnp.where(high_code == (line >> shift), 1.0, 0.0).astype(bf16)
        count = count + lax.dot_general(
            high, low, (((1,), (1,)), ((), ())), preferred_element_type=f32
        )
    cnt_ref[...] = count
    for p in range(half):
        tails_ref[p] = tail_rows(count[half + p : half + p + 1])


def segment_kernel(
    hid_ref, near_ref, far_ref, gain_ref, hot_ref, tails_ref, act_ref, send_ref, acc_ref
):
    clips, tokens, channels = hid_ref.shape
    members = tokens * (channels // GROUPS)
    gain = gain_ref[...]
    block = 64
    for c in range(clips):
        mean, inverse = merged(
            near_ref[c : c + 1],
            near_ref[clips + c : clips + c + 1],
            far_ref[c : c + 1],
            far_ref[clips + c : clips + c + 1],
            members,
        )
        scale = inverse * gain
        for i in range(tokens // block):
            x = hid_ref[c, i * block : (i + 1) * block]
            act = silu((x - mean) * scale).astype(bf16)
            act_ref[c * tokens + i * block : c * tokens + (i + 1) * block] = act

    share = LANES
    half = SHARDS // 2
    acc_ref[...] = jnp.dot(hot_ref[...], act_ref[...], preferred_element_type=f32)
    for p in range(half):
        send_ref[p, :share] = acc_ref[p * share : (p + 1) * share].astype(bf16)
        send_ref[p, share:] = tails_ref[p]


def keep_kernel(act_ref, codes_ref, keep_ref):
    hot_rows(codes_ref, act_ref, keep_ref, 0)


def quarter_kernel(keep_ref, cnt_ref, got_ref, mine_ref, mcnt_ref, s1_ref, s2_ref, s3_ref):
    share = LANES
    for p, out in enumerate((None, s1_ref, s2_ref, s3_ref)):
        value = keep_ref[p * share : (p + 1) * share] + got_ref[p, :share].astype(f32)
        count = cnt_ref[p : p + 1] + untail(got_ref[p, share:])
        if out is None:
            mine_ref[...] = value
            mcnt_ref[...] = jnp.broadcast_to(count, (8, LANES))
        else:
            out[:share] = value.astype(bf16)
            out[share:] = tail_rows(count)


def gathered_kernel(mine_ref, mcnt_ref, a_ref, b_ref, c_ref, after_ref, out_ref):
    share = mine_ref.shape[0]
    value = mine_ref[...]
    count = mcnt_ref[0:1]
    for ref in (a_ref, b_ref, c_ref):
        value = value + ref[:share].astype(f32)
        count = count + untail(ref[share:])
    out_ref[:share] = value.astype(bf16)
    out_ref[share:] = tail_rows(count)


def pair_kernel(own_ref, got_ref, out_ref):
    share = own_ref.shape[0] - TAIL
    value = own_ref[:share].astype(f32) + got_ref[:share].astype(f32)
    out_ref[:share] = value.astype(bf16)
    out_ref[share:] = tail_rows(untail(own_ref[share:]) + untail(got_ref[share:]))


def project_kernel(own_ref, got_ref, w_ref, err_ref, out_ref):
    share = own_ref.shape[0] - TAIL
    value = own_ref[:share].astype(f32) + got_ref[:share].astype(f32)
    head = value.astype(bf16)
    rest = (value - head.astype(f32)).astype(bf16)
    sums = jnp.dot(head, w_ref[...], preferred_element_type=f32) + jnp.dot(
        rest, w_ref[...], preferred_element_type=f32
    )
    out_ref[:share] = sums.astype(bf16)
    out_ref[share:] = tail_rows(
        untail(own_ref[share:]) + untail(got_ref[share:]), err_ref[0:1]
    )


def as_column(row):
    return jnp.transpose(jnp.broadcast_to(row, (LANES, LANES)))


def latent_kernel(act_ref, w_ref, codes_ref, sum_ref, cnt_ref, after_ref, lat_ref, err_ref, head_ref, rest_ref):
    tokens, channels = lat_ref.shape
    codes_count = sum_ref.shape[0]
    clips = 2
    counts = cnt_ref[...]
    grand = jnp.sum(counts)
    smooth = (counts + smooth_eps) / (grand + codes_count * smooth_eps) * grand
    for i in range(codes_count // LANES):
        divisor = as_column(smooth[i : i + 1])
        divisor = jnp.concatenate([divisor] * (channels // LANES), axis=1)
        book = sum_ref[i * LANES : (i + 1) * LANES] / divisor
        head = book.astype(bf16)
        head_ref[i * LANES : (i + 1) * LANES] = head
        rest_ref[i * LANES : (i + 1) * LANES] = (book - head.astype(f32)).astype(bf16)
    lane_code = lax.broadcasted_iota(jnp.int32, (LANES, codes_count), 1)
    lane = lax.broadcasted_iota(jnp.int32, (1, LANES), 1)
    lines = tokens // LANES
    per_clip = lines // clips
    errors = jnp.zeros((1, LANES), f32)
    for c in range(clips):
        def step(i, acc):
            line = c * per_clip + i
            at = pl.ds(pl.multiple_of(line * LANES, LANES), LANES)
            latent = jnp.dot(act_ref[at], w_ref[...], preferred_element_type=f32)
            lat_ref[at] = latent
            column = as_column(codes_ref[pl.ds(line, 1)])
            column = jnp.concatenate([column] * (codes_count // LANES), axis=1)
            hot = jnp.where(column == lane_code, 1.0, 0.0).astype(bf16)
            chosen = jnp.dot(hot, head_ref[...], preferred_element_type=f32) + jnp.dot(
                hot, rest_ref[...], preferred_element_type=f32
            )
            away = latent - chosen
            away = away * away
            return acc + jnp.sum(away.reshape(LANES // 8, 8, channels), axis=0)

        total = lax.fori_loop(0, per_clip, step, jnp.zeros((8, channels), f32), unroll=True)
        errors = jnp.where(lane == c, jnp.sum(total), errors)
    err_ref[...] = jnp.broadcast_to(errors, (8, LANES))


def book_kernel(first, tokens, *refs, done=lambda: None):
    parts, (sum_ref, cnt_ref), rest = refs[:-8], refs[-8:-6], refs[-6:]
    _, _, book_hbm, count_ref, page_ref, sems = rest
    me = shard_bits()
    share = LANES
    channels = sum_ref.shape[1]
    grand = ema_decay * jnp.sum(cnt_ref[...]) + (1.0 - ema_decay) * tokens
    copies = []
    for i in range(SHARDS // 2):
        src = parts[i] if len(parts) > 1 else parts[0].at[i]
        shard = (first + i) ^ me
        count = ema_decay * cnt_ref[pl.ds(shard, 1)] + (1.0 - ema_decay) * untail(src[share:])
        count_ref[i : i + 1] = count
        smooth = (count + smooth_eps) / (grand + SHARDS * share * smooth_eps) * grand
        inverse = as_column(1.0 / smooth)
        inverse = jnp.concatenate([inverse] * (channels // LANES), axis=1)
        at = pl.ds(pl.multiple_of(shard * share, share), share)
        fresh = ema_decay * sum_ref[at] + (1.0 - ema_decay) * src[:share].astype(f32)
        page_ref[i] = fresh * inverse
        copies.append(pltpu.make_async_copy(page_ref.at[i], book_hbm.at[at], sems.at[i]))
        copies[-1].start()
    done()
    for copy in copies:
        copy.wait()


def early_kernel(
    tokens, scale, p0, p1, p2, p3, sum_ref, cnt_ref, err_ref, book_hbm, count_ref, error_hbm, page_ref, error_ref, sems
):
    copy = pltpu.make_async_copy(error_ref, error_hbm, sems.at[SHARDS // 2])
    errors = (err_ref[0:1] + untail(p1[LANES:], 1)) * scale
    error_ref[...] = errors[0, : error_ref.shape[0]]
    copy.start()
    book_kernel(0, tokens, p0, p1, p2, p3, sum_ref, cnt_ref, None, None, book_hbm, count_ref, page_ref, sems)
    copy.wait()


def late_kernel(
    tokens, q0, q1, q2, q3, sum_ref, cnt_ref, book_in, early_ref, book_hbm, count_hbm, page_ref, late_ref, line_ref, sems
):
    half = SHARDS // 2
    copy = pltpu.make_async_copy(line_ref, count_hbm, sems.at[half])

    def counts():
        me = shard_bits()
        for i in range(half):
            line_ref[pl.ds(i ^ me, 1)] = early_ref[i : i + 1]
            line_ref[pl.ds((half + i) ^ me, 1)] = late_ref[i : i + 1]
        copy.start()

    book_kernel(
        half, tokens, q0, q1, q2, q3, sum_ref, cnt_ref, None, None, book_hbm, late_ref, page_ref, sems, done=counts
    )
    copy.wait()


def body(video, gain_first, conv_weight, gain_second, proj_weight, codes, ema_sum, ema_count):
    clips, frames, rows, cols, channels = video.shape
    codes_count = ema_sum.shape[0]
    clip_size, strips = lax.axis_size("clip"), lax.axis_size("strip")
    n = clip_size * strips
    share = codes_count // SHARDS
    assert strips == 2 and clip_size >= 4 and clip_size & (clip_size - 1) == 0
    assert share == LANES and channels == 2 * LANES and clips == 2

    def swap(x, mask):
        return lax.ppermute(x, BOTH, [(i, i ^ mask) for i in range(n)])

    tokens = frames * rows * cols
    halo = clips * frames * cols
    pay, near, held = call(
        stats_kernel,
        [
            ((halo + 16, channels), bf16),
            ((8, channels), f32),
            (video.shape, bf16),
        ],
        [pltpu.with_memory_space_constraint(video, pltpu.HBM)],
        scratch=[pltpu.SemaphoreType.DMA((clips,))],
        flops=10_000_000,
        limit=16 << 20,
        name="stats",
        far=(0,),
    )
    far_pay = swap(pay, 1)
    weights = pltpu.with_memory_space_constraint(
        conv_weight.reshape(3, 9 * channels, channels), pltpu.HBM
    )
    (taps,) = call(
        taps_kernel,
        [((min(3, frames), 9 * channels, channels), bf16)],
        [weights, near],
        scratch=[pltpu.SemaphoreType.DMA((1,))],
        flops=1_000_000_000,
        limit=8 << 20,
        name="taps",
        far=(0,),
    )
    hidden, near_two = call(
        conv_kernel,
        [((clips, tokens, channels), f32), ((8, channels), f32)],
        [held, far_pay, near, gain_first.reshape(1, channels), taps],
        scratch=[VMEM((clips, frames, rows + 2, cols, 3 * channels), bf16)],
        flops=4_000_000_000,
        limit=24 << 20,
        name="conv",
    )
    code_lines = lax.optimization_barrier((codes, near_two))[0].reshape(-1, LANES)
    far_two = swap(near_two, 1)
    cnt, tails, hot = call(
        count_kernel,
        [
            ((SHARDS, LANES), f32),
            ((SHARDS // 2, TAIL, channels), bf16),
            ((codes_count // 2, clips * tokens), bf16),
        ],
        [code_lines, near_two],
        flops=500_000_000,
        limit=8 << 20,
        name="count",
    )
    act, send = call(
        segment_kernel,
        [
            ((clips * tokens, channels), bf16),
            ((SHARDS // 2, share + TAIL, channels), bf16),
        ],
        [hidden, near_two, far_two, gain_second.reshape(1, channels), hot, tails],
        scratch=[VMEM((codes_count // 2, channels), f32)],
        flops=1_500_000_000,
        limit=24 << 20,
        name="segment",
    )
    core, x_bit = 2, 4
    got = swap(send, core)
    (keep,) = call(
        keep_kernel,
        [((codes_count // 2, channels), f32)],
        [act, code_lines],
        flops=1_000_000_000,
        limit=8 << 20,
        name="keep",
    )
    counts = ema_count.reshape(SHARDS, LANES)
    flat = ((share + TAIL, channels), bf16)
    mine, mine_cnt, s1, s2, s3 = call(
        quarter_kernel,
        [((share, channels), f32), ((8, LANES), f32), flat, flat, flat],
        [keep, cnt, got],
        flops=1_000_000,
        limit=8 << 20,
        name="quarter",
    )
    near_masks = (1, x_bit, 1 | x_bit)
    parts = [swap(s, m) for s, m in zip((s1, s2, s3), near_masks)]
    latent, err = call(
        latent_kernel,
        [((clips * tokens, channels), f32), ((8, LANES), f32)],
        [act, proj_weight, code_lines, ema_sum, counts, mine_cnt],
        scratch=[VMEM((codes_count, channels), bf16)] * 2,
        flops=2_500_000_000,
        limit=24 << 20,
        name="latent",
    )
    (own,) = call(
        gathered_kernel, [flat], [mine, mine_cnt, *parts, err], flops=1_000_000, limit=8 << 20, name="gathered"
    )
    bit = 8
    while bit < n // 2:
        (own,) = call(
            pair_kernel, [flat], [own, swap(own, bit)], flops=1_000_000, limit=8 << 20, name="pair"
        )
        bit *= 2
    last = swap(own, bit) if bit < n else jnp.zeros_like(own)
    (done,) = call(
        project_kernel, [flat], [own, last, proj_weight, err], flops=1_000_000, limit=8 << 20, name="project"
    )
    peers = [swap(done, m) for m in near_masks]
    across = [swap(part, core) for part in (done, *peers)]
    scale = 1.0 / (tokens * strips * channels)
    total_tokens = float(clips * tokens * n)
    half = SHARDS // 2
    page = VMEM((half, share, channels), f32)
    book_shape = ((codes_count, channels), f32)
    book, early, error = call(
        functools.partial(early_kernel, total_tokens, scale),
        [book_shape, ((8, LANES), f32), ((clips,), f32)],
        [done, *peers, ema_sum, counts, err],
        scratch=[page, VMEM((clips,), f32), pltpu.SemaphoreType.DMA((half + 1,))],
        flops=1_000_000,
        limit=8 << 20,
        name="early",
        far_outs=(0, 2),
    )
    book, count = call(
        functools.partial(late_kernel, total_tokens),
        [book_shape, ((SHARDS, LANES), f32)],
        [*across, ema_sum, counts, book, early],
        scratch=[
            page,
            VMEM((8, LANES), f32),
            VMEM((SHARDS, LANES), f32),
            pltpu.SemaphoreType.DMA((half + 1,)),
        ],
        flops=1_000_000,
        limit=8 << 20,
        name="late",
        far=(half + 2,),
        far_outs=(0, 1),
        alias={half + 2: 0},
    )
    return (
        latent.reshape(clips, frames, rows, cols, channels),
        book,
        count.reshape(codes_count),
        error,
    )


def solution(mesh):
    in_specs = (
        P("clip", None, "strip", None, None),
        P(),
        P(),
        P(),
        P(),
        P("clip", None, "strip", None),
        P(),
        P(),
    )
    out_specs = (P("clip", None, "strip", None, None), P(), P(), P("clip"))
    return jax.shard_map(body, mesh=mesh, in_specs=in_specs, out_specs=out_specs, check_vma=False)
```
